32 devices in a mesh: grp: 8 (over z, x), brick: 4 (over y, core).
Axes of the slice: x: 2, y: 2, z: 4, core: 2. Of those that a mesh axis runs over, the one named last changes fastest.
Arguments:
- deformation_vector: float32 [3, 32, 64, 256], P(None, 'grp', 'brick'), may hold values from -4 to 4
- applied_traction: float32 [3, 32, 64, 256], P(None, 'grp', 'brick'), may hold values from 4 to 16
- heat_level: float32 [32, 64, 256], P('grp', 'brick'), may hold values from -6 to 6
- stiffness_main_terms: float32 [3, 32, 64, 256], P(None, 'grp', 'brick'), may hold values from 8 to 10
- stiffness_cross_terms: float32 [3, 32, 64, 256], P(None, 'grp', 'brick'), may hold values from -0.8 to 0.8
- normal_clearance: float32 [32, 64, 256], P('grp', 'brick'), may hold values from -0.5 to 1
- touching_flag: int32 [32, 64, 256], P('grp', 'brick'), may hold values 0 or 1
- clipped_normal_flag: int32 [32, 64, 256], P('grp', 'brick'), may hold values 0 or 1
Outputs:
- moved: float32 [3, 32, 64, 256], P(None, 'grp', 'brick')
- residual: float32 [3, 32, 64, 256], P(None, 'grp', 'brick')
The draws below stay inside these ranges and needn't reach their ends.
All inputs are finite; a program needn't handle non-finite values. No bound on the sum of `touching_flag` or of `clipped_normal_flag` on one device may be relied on, other than what follows from the above.
Results may differ from the reference program's by a relative error of at most 0.00002.
Values sent between devices are 32-bit elements; how exact they have to be, the bound alone decides.
A program may use at most 128 MiB of HBM per device.

```python
import jax
import jax.numpy as jnp

POINTS_ALONG_X = 32
POINTS_ALONG_Y = 64
POINTS_ALONG_Z = 256


def set_ends(entries, own_key, least, largest):
    longest = entries.shape.index(max(entries.shape))
    spots = []
    for shift in (0, 1):
        where = [jax.random.randint(jax.random.fold_in(own_key, axis), (), 0, length) for axis, length in enumerate(entries.shape)]
        where[longest] = (where[longest] + shift) % entries.shape[longest]
        spots.append(tuple(where))
    return entries.at[spots[0]].set(least).at[spots[1]].set(largest)


def levels(stream_key, dims, pieces, smallest, largest):
    gain, own = 1.0, jax.random.fold_in(stream_key, 6)
    for position, shards_of in pieces:
        draws = jnp.exp(jax.random.uniform(jax.random.fold_in(own, position), (shards_of,), jnp.float32, smallest / len(pieces), largest / len(pieces)))
        gain = gain * jnp.repeat(draws, dims[position] // shards_of).reshape([-1 if axis == position else 1 for axis in range(len(dims))])
    return gain


def normal_values(own_key, dims, deviation, reach, cuts=(), kind=jnp.bfloat16):
    result = deviation * jax.random.normal(own_key, dims, jnp.float32)
    if cuts:
        result = result * levels(own_key, dims, cuts, -0.22, 0.18)
    return jnp.clip(result, -reach, reach).astype(kind)


def setup_inputs(seed: int = 0) -> dict:
    arg_keys = jax.random.split(jax.random.key(seed), 9)
    return {
        "deformation_vector": normal_values(arg_keys[0], (3, POINTS_ALONG_X, POINTS_ALONG_Y, POINTS_ALONG_Z), 0.5, 4.0, ((1, 8), (2, 4)), jnp.float32),
        "applied_traction": jnp.clip(4.0 + 12.0 * jax.random.uniform(arg_keys[1], (3, POINTS_ALONG_X, POINTS_ALONG_Y, POINTS_ALONG_Z), jnp.float32) ** levels(arg_keys[1], (3, POINTS_ALONG_X, POINTS_ALONG_Y, POINTS_ALONG_Z), ((1, 8), (2, 4)), -0.2, 0.2), 4.0, 16.0),
        "heat_level": normal_values(arg_keys[2], (POINTS_ALONG_X, POINTS_ALONG_Y, POINTS_ALONG_Z), 1.0, 6.0, ((0, 8), (1, 4)), jnp.float32),
        "stiffness_main_terms": jnp.clip(8.0 + 2.0 * jax.random.uniform(arg_keys[3], (3, POINTS_ALONG_X, POINTS_ALONG_Y, POINTS_ALONG_Z), jnp.float32) ** levels(arg_keys[3], (3, POINTS_ALONG_X, POINTS_ALONG_Y, POINTS_ALONG_Z), ((1, 8), (2, 4)), -0.2, 0.2), 8.0, 10.0),
        "stiffness_cross_terms": jnp.clip(jax.random.uniform(arg_keys[4], (3, POINTS_ALONG_X, POINTS_ALONG_Y, POINTS_ALONG_Z), jnp.float32, -0.8, 0.8) * levels(arg_keys[4], (3, POINTS_ALONG_X, POINTS_ALONG_Y, POINTS_ALONG_Z), ((1, 8), (2, 4)), -0.4, 0.0), -0.8, 0.8),
        "normal_clearance": jnp.clip(-0.5 + 1.5 * jax.random.uniform(arg_keys[5], (POINTS_ALONG_X, POINTS_ALONG_Y, POINTS_ALONG_Z), jnp.float32) ** levels(arg_keys[5], (POINTS_ALONG_X, POINTS_ALONG_Y, POINTS_ALONG_Z), ((0, 8), (1, 4)), -0.2, 0.2), -0.5, 1.0),
        "touching_flag": set_ends((jax.random.randint(arg_keys[6], (POINTS_ALONG_X, POINTS_ALONG_Y, POINTS_ALONG_Z), 0, 3) < 1).astype(jnp.int32), jax.random.fold_in(arg_keys[6], 1), 0, 1),
        "clipped_normal_flag": set_ends((jax.random.randint(arg_keys[7], (POINTS_ALONG_X, POINTS_ALONG_Y, POINTS_ALONG_Z), 0, 2) < 1).astype(jnp.int32), jax.random.fold_in(arg_keys[7], 1), 0, 1),
    }


OMEGA = 0.6
FREE = 1000.0


def block_times(diag, off, field):
    a, b, c = diag[0], diag[1], diag[2]
    d, e, f = off[0], off[1], off[2]
    return jnp.stack([a * field[0] + d * field[1] + f * field[2],
                      d * field[0] + b * field[1] + e * field[2],
                      f * field[0] + e * field[1] + c * field[2]])


def inverse_entries(diag, off):
    a, b, c = diag[0], diag[1], diag[2]
    d, e, f = off[0], off[1], off[2]
    i00 = b * c - e * e
    i11 = a * c - f * f
    i22 = a * b - d * d
    i01 = f * e - d * c
    i12 = d * f - a * e
    i02 = d * e - b * f
    scale = 1.0 / (a * i00 + d * i01 + f * i02)
    return jnp.stack([i00 * scale, i11 * scale, i22 * scale, i01 * scale, i12 * scale, i02 * scale])


def inverse_times(inv, rest):
    return jnp.stack([inv[0] * rest[0] + inv[3] * rest[1] + inv[5] * rest[2],
                      inv[3] * rest[0] + inv[1] * rest[1] + inv[4] * rest[2],
                      inv[5] * rest[0] + inv[4] * rest[1] + inv[2] * rest[2]])


def operate(field, diag, off):
    padded = jnp.pad(field, ((0, 0), (1, 1), (1, 1), (1, 1)))
    beside = padded[:, 2:, 1:-1, 1:-1] + padded[:, :-2, 1:-1, 1:-1]
    beside = beside + padded[:, 1:-1, 2:, 1:-1] + padded[:, 1:-1, :-2, 1:-1]
    beside = beside + padded[:, 1:-1, 1:-1, 2:] + padded[:, 1:-1, 1:-1, :-2]
    return block_times(diag, off, field) - beside


def project(field, obstacle):
    return jnp.concatenate([jnp.minimum(field[0], obstacle)[None], field[1:]], 0)


def sweep(field, force, diag, off, inv, obstacle):
    rest = force - operate(field, diag, off)
    return project(field + OMEGA * inverse_times(inv, rest), obstacle)


def grouped(x):
    s = x.shape
    return x.reshape(s[:-3] + (s[-3] // 2, 2, s[-2] // 2, 2, s[-1] // 2, 2))


def group_sum(x):
    return jnp.sum(grouped(x), axis=(-5, -3, -1))


def group_min(x):
    return jnp.min(grouped(x), axis=(-5, -3, -1))


def spread(x):
    return jnp.repeat(jnp.repeat(jnp.repeat(x, 2, axis=-3), 2, axis=-2), 2, axis=-1)


def reference(deformation_vector, applied_traction, heat_level, stiffness_main_terms, stiffness_cross_terms, normal_clearance, touching_flag, clipped_normal_flag):
    heating_traction = jnp.pad(heat_level, 1)
    drift = jnp.stack([heating_traction[2:, 1:-1, 1:-1] - heating_traction[:-2, 1:-1, 1:-1],
                       heating_traction[1:-1, 2:, 1:-1] - heating_traction[1:-1, :-2, 1:-1],
                       heating_traction[1:-1, 1:-1, 2:] - heating_traction[1:-1, 1:-1, :-2]])
    force = applied_traction - drift
    inv1 = inverse_entries(stiffness_main_terms, stiffness_cross_terms)
    obstacle1 = jnp.where(touching_flag == 1, normal_clearance, FREE)
    field = sweep(deformation_vector, force, stiffness_main_terms, stiffness_cross_terms, inv1, obstacle1)
    field = sweep(field, force, stiffness_main_terms, stiffness_cross_terms, inv1, obstacle1)
    rest = force - operate(field, stiffness_main_terms, stiffness_cross_terms)
    rest = jnp.concatenate([jnp.where(clipped_normal_flag == 1, 0.0, rest[0])[None], rest[1:]], 0)
    force2 = 0.25 * group_sum(rest)
    diag2 = 0.125 * group_sum(stiffness_main_terms)
    off2 = 0.125 * group_sum(stiffness_cross_terms)
    allowed = (touching_flag == 1) & (clipped_normal_flag == 0)
    obstacle2 = group_min(jnp.where(allowed, normal_clearance - field[0], FREE))
    inv2 = inverse_entries(diag2, off2)
    middle = jnp.zeros_like(force2)
    middle = sweep(middle, force2, diag2, off2, inv2, obstacle2)
    middle = sweep(middle, force2, diag2, off2, inv2, obstacle2)
    force3 = 0.25 * group_sum(force2 - operate(middle, diag2, off2))
    diag3 = 0.125 * group_sum(diag2)
    off3 = 0.125 * group_sum(off2)
    obstacle3 = group_min(obstacle2 - middle[0])
    inv3 = inverse_entries(diag3, off3)
    lowest = jnp.zeros_like(force3)
    lowest = sweep(lowest, force3, diag3, off3, inv3, obstacle3)
    lowest = sweep(lowest, force3, diag3, off3, inv3, obstacle3)
    middle = middle + spread(lowest)
    middle = sweep(middle, force2, diag2, off2, inv2, obstacle2)
    middle = sweep(middle, force2, diag2, off2, inv2, obstacle2)
    correction = spread(middle)
    correction = jnp.concatenate([jnp.where(clipped_normal_flag == 1, 0.0, correction[0])[None], correction[1:]], 0)
    field = field + correction
    field = sweep(field, force, stiffness_main_terms, stiffness_cross_terms, inv1, obstacle1)
    field = sweep(field, force, stiffness_main_terms, stiffness_cross_terms, inv1, obstacle1)
    residual = force - operate(field, stiffness_main_terms, stiffness_cross_terms)
    return field, residual
```

```python
import jax
import jax.numpy as jnp
from jax import lax
from jax.experimental import pallas as pl
from jax.experimental.pallas import tpu as pltpu
from jax.sharding import PartitionSpec as P

OMEGA = 0.6
FREE = 1000.0
EXCHANGES = 11
FINE = (0, 1, 2, 8, 9, 10)
DEPTH = {3: 3, 4: 2, 5: 1, 6: 2}
USED = FINE + tuple(DEPTH)
TWICE = (3, 6)
PIECES = 2
MESH = pl.DeviceIdType.MESH


def inverse(k):
    a, b, c, d, e, f = k
    i00 = b * c - e * e
    i11 = a * c - f * f
    i22 = a * b - d * d
    i01 = f * e - d * c
    i12 = d * f - a * e
    i02 = d * e - b * f
    scale = 1.0 / (a * i00 + d * i01 + f * i02)
    return [i00 * scale, i11 * scale, i22 * scale, i01 * scale, i12 * scale, i02 * scale]


def symmetric_times(m, v):
    return [
        m[0] * v[0] + m[3] * v[1] + m[5] * v[2],
        m[3] * v[0] + m[1] * v[1] + m[4] * v[2],
        m[5] * v[0] + m[4] * v[1] + m[2] * v[2],
    ]


def kernel(
    disp_h, load_h, heat_h, diag_h, off_h, clear_h, touch_h, clip_h,
    moved, resid,
    first, heat, fine, edge, middle, xs, xr, ys, yr, ds, dr, halo_x, halo_y, load, stiff, clear, touch, clip,
    force, rests, inv1, obst1, g2, k2, inv2, obst2, g3, k3, inv3, obst3,
    in_sem, send_sem, recv_sem, dsend_sem, drecv_sem,
):
    X, Y, Z = heat_h.shape
    X2, X3 = X // 2, X // 4
    H = Y // PIECES
    g, b = lax.axis_index("grp"), lax.axis_index("brick")
    ng, nb = lax.axis_size("grp"), lax.axis_size("brick")
    ways = (
        ("grp", g - 1, g > 0),
        ("grp", g + 1, g < ng - 1),
        ("brick", b - 1, b > 0),
        ("brick", b + 1, b < nb - 1),
    )
    barrier = pltpu.get_barrier_semaphore()
    for axis, there, has in ways:

        @pl.when(has)
        def _():
            pl.semaphore_signal(barrier, inc=1, device_id={axis: there}, device_id_type=MESH)

    corners = [
        (ways[p][1], ways[2 + q][1], ways[p][2] & ways[2 + q][2]) for p in (0, 1) for q in (0, 1)
    ]
    for at, beyond, has in corners:

        @pl.when(has)
        def _():
            pl.semaphore_signal(
                barrier, inc=1, device_id={"grp": at, "brick": beyond}, device_id_type=MESH
            )

    pairs = (
        (disp_h, first.at[:, 1 : X + 1]),
        (heat_h, heat),
        (diag_h, stiff.at[0:3]),
        (off_h, stiff.at[3:6]),
        (load_h, load),
        (clear_h, clear),
        (touch_h, touch),
        (clip_h, clip),
    )
    arriving = [pltpu.make_async_copy(s, d, in_sem.at[i]) for i, (s, d) in enumerate(pairs)]
    for copy in arriving:
        copy.start()

    row = lax.broadcasted_iota(jnp.int32, (Y, Z), 0)
    lane = lax.broadcasted_iota(jnp.int32, (Y, Z), 1)
    lanes = {8: lax.broadcasted_iota(jnp.int32, (8, Z), 1), Y: lane}
    even_row = (row & 1) == 0
    even_lane = (lane & 1) == 0

    def fine_ref(k):
        return first if k == 0 else fine.at[FINE.index(k) - 1]

    for way, (axis, there, has) in enumerate(ways):

        @pl.when(jnp.logical_not(has))
        def _():
            for k in USED:
                if way >= 2:
                    yr[k, way - 2] = jnp.zeros(yr.shape[2:], jnp.float32)
                elif k in FINE:
                    for c in range(3):
                        fine_ref(k)[c, 0 if way == 0 else X + 1] = jnp.zeros((Y, Z), jnp.float32)
                else:
                    for n in range(DEPTH[k]):
                        xr[k, way, n] = jnp.zeros((Y, Z), jnp.float32)

    for n, (_, _, has) in enumerate(corners):

        @pl.when(jnp.logical_not(has))
        def _():
            for k in range(2):
                dr[k, n] = jnp.zeros((8, Z), jnp.float32)

    def rows_of(k):
        count = 4 * X if k == 0 else 3 * X if k in FINE else {3: 10, 4: 6, 5: 3, 6: 6}[k] * X2
        return -(-count // 8) * 8

    def transfer(k, way, p=0):
        if way >= 2:
            n = way - 2
            src, dst = ys.at[k, n, 0 : rows_of(k)], yr.at[k, 1 - n, 0 : rows_of(k)]
        elif k in FINE:
            part = pl.ds(p * H, H)
            src = edge.at[FINE.index(k), way, :, part]
            dst = fine_ref(k).at[:, 0 if way else X + 1, part]
        else:
            src, dst = xs.at[k, way, 0 : DEPTH[k]], xr.at[k, 1 - way, 0 : DEPTH[k]]
        axis, there, _ = ways[way]
        return pltpu.make_async_remote_copy(
            src_ref=src,
            dst_ref=dst,
            send_sem=send_sem.at[k, way, p],
            recv_sem=recv_sem.at[k, way ^ 1, p],
            device_id={axis: there},
            device_id_type=MESH,
        )

    def begin(k, sides=(0, 1, 2, 3), p=0):
        for way in sides:

            @pl.when(ways[way][2])
            def _():
                transfer(k, way, p).start()

    def arrive(k, sides, p=0):
        for side in sides:

            @pl.when(ways[side][2])
            def _():
                transfer(k, side ^ 1, p).wait_recv()

    def leave(k):
        for way in range(4):

            @pl.when(ways[way][2])
            def _():
                for p in range(PIECES if k in FINE and way < 2 else 1):
                    transfer(k, way, p).wait_send()

    def cross(k, n):
        at, beyond, _ = corners[n]
        return pltpu.make_async_remote_copy(
            src_ref=ds.at[TWICE.index(k), n],
            dst_ref=dr.at[TWICE.index(k), 3 - n],
            send_sem=dsend_sem.at[TWICE.index(k), n],
            recv_sem=drecv_sem.at[TWICE.index(k), 3 - n],
            device_id={"grp": at, "brick": beyond},
            device_id_type=MESH,
        )

    def cross_all(k, what):
        for n in range(4):

            @pl.when(corners[3 - n if what == "arrive" else n][2])
            def _():
                copy = cross(k, n)
                if what == "begin":
                    copy.start()
                elif what == "arrive":
                    copy.wait_recv()
                else:
                    copy.wait_send()

    def edge_rows(k, layers, c, i, v):
        n = c * layers + i
        ys[k, 0, n : n + 1, :] = v[0:1, :]
        ys[k, 1, n : n + 1, :] = v[Y - 1 : Y, :]

    def before(v, s):
        return jnp.where(lanes[v.shape[0]] < s, 0.0, pltpu.roll(v, s, 1))

    def after(v, s):
        return jnp.where(lanes[v.shape[0]] >= Z - s, 0.0, pltpu.roll(v, Z - s, 1))

    def above(k, layers, c, i, v, s):
        n = c * layers + i
        return jnp.where(row < s, yr[k, 0, n : n + 1, :], pltpu.roll(v, s, 0))

    def below(k, layers, c, i, v, s):
        n = c * layers + i
        return jnp.where(row >= Y - s, yr[k, 1, n : n + 1, :], pltpu.roll(v, Y - s, 0))

    def pair_lane(v, s, how):
        return how(v, jnp.where((lane & s) == 0, pltpu.roll(v, Z - s, 1), pltpu.roll(v, s, 1)))

    def pair_row(v, s, how):
        return how(v, jnp.where((row & s) == 0, pltpu.roll(v, Y - s, 0), pltpu.roll(v, s, 0)))

    def group(v, w, s, how):
        return pair_row(pair_lane(how(v, w), s, how), s, how)

    def plus(v, w):
        return v + w

    def pack(v):
        odd = v[2] if len(v) == 3 else jnp.where(even_row, v[2], v[3])
        return jnp.where(even_lane, jnp.where(even_row, v[0], v[1]), odd)

    def split(q):
        return [
            jnp.where(even_row, q, pltpu.roll(q, 1, 0)),
            jnp.where(even_row, pltpu.roll(q, Y - 1, 0), q),
        ]

    def unpack(p, four=False):
        odd = jnp.where(even_lane, pltpu.roll(p, Z - 1, 1), p)
        return split(jnp.where(even_lane, p, pltpu.roll(p, 1, 1))) + (split(odd) if four else [odd])

    def layer(ref, i, count=3):
        return [ref[c, i] for c in range(count)]

    def put(ref, i, values):
        for c, v in enumerate(values):
            ref[c, i] = v

    def stage(k, layers, s, value, blocks, right, halo, finish):
        if k > 0:
            arrive(k, (2, 3))

        def partial(i):
            v = value(i)
            kv = symmetric_times(blocks(i), v)
            g = right(i)
            rest = []
            for c in range(3):
                near = above(k, layers, c, i, v[c], s) + below(k, layers, c, i, v[c], s)
                near = near + (before(v[c], s) + after(v[c], s))
                rest.append((g[c] - kv[c]) + near)
            for n in (i - 1, i + 1):
                if 0 <= n < layers:
                    rest = [r + x for r, x in zip(rest, value(n))]
            return rest

        for i in range(1, layers - 1):
            finish(i, value(i), partial(i))
        ends = {i: partial(i) for i in {0, layers - 1}}
        for side, i in ((0, 0), (1, layers - 1)):
            arrive(k, (side,))
            ends[i] = [r + x for r, x in zip(ends[i], halo(side))]
            if side == 1 or layers > 1:
                finish(i, value(i), ends[i])

    def relaxed(v, inv, rest, obstacle):
        step = symmetric_times(inv, rest)
        w = [v[c] + OMEGA * step[c] for c in range(3)]
        return [jnp.minimum(w[0], obstacle), w[1], w[2]]

    def opened(inv, right, obstacle):
        w = [OMEGA * x for x in symmetric_times(inv, right)]
        return [jnp.minimum(w[0], obstacle), w[1], w[2]]

    def fine_stage(k, finish):
        ref = fine_ref(k)
        for i in range(X):
            v = layer(ref, i + 1)
            kv = symmetric_times(layer(stiff, i, 6), v)
            for c in range(3):
                near = jnp.where(row < 1, 0.0, pltpu.roll(v[c], 1, 0))
                near = near + jnp.where(row >= Y - 1, 0.0, pltpu.roll(v[c], Y - 1, 0))
                near = near + (before(v[c], 1) + after(v[c], 1))
                r = (force[c, i] - kv[c]) + near
                for n in (i - 1, i + 1):
                    if 0 <= n < X:
                        r = r + ref[c, n + 1]
                rests[c, i] = r
        if k > 0:
            arrive(k, (2, 3))
        for i in range(X):
            for c in range(3):
                n = c * X + i
                rests[c, i, 0:1, :] = rests[c, i, 0:1, :] + yr[k, 0, n : n + 1, :]
                rests[c, i, Y - 1 : Y, :] = rests[c, i, Y - 1 : Y, :] + yr[k, 1, n : n + 1, :]
        for i in range(1, X - 1):
            for p in range(PIECES):
                finish(i, p, [rests[c, i, pl.ds(p * H, H)] for c in range(3)])
        for p in range(PIECES):
            part = pl.ds(p * H, H)
            for side, i in ((0, 0), (1, X - 1)):
                arrive(k, (side,), p)
                rest = [rests[c, i, part] + ref[c, (X + 1) * side, part] for c in range(3)]
                if X == 1 and side == 0:
                    for c in range(3):
                        rests[c, i, part] = rest[c]
                else:
                    finish(i, p, rest)

    def leave_edge(k, side, p, w):
        part = pl.ds(p * H, H)
        h = heat[(X - 1) * side, part]
        edge[FINE.index(k), side, 0, part] = w[0] + h if side else w[0] - h
        for c in (1, 2):
            edge[FINE.index(k), side, c, part] = w[c]
        begin(k, (side,), p)

    def fine_store(to, i, p, w):
        for c in range(3):
            fine_ref(to)[c, i + 1, pl.ds(p * H, H)] = w[c]
        for side, end in ((0, 0), (1, X - 1)):
            if i == end:
                leave_edge(to, side, p, w)
        for c in range(3):
            n = c * X + i
            if p == 0:
                ys[to, 0, n : n + 1, :] = w[c][0:1, :]
            if p == PIECES - 1:
                ys[to, 1, n : n + 1, :] = w[c][H - 1 : H, :]

    def fine_sweep(k, to):
        def finish(i, p, rest):
            part = pl.ds(p * H, H)
            v = [fine_ref(k)[c, i + 1, part] for c in range(3)]
            w = relaxed(v, [inv1[c, i, part] for c in range(6)], rest, obst1[i, part])
            fine_store(to, i, p, w)
            if to == 10:
                for c in range(3):
                    moved[c, i, part] = w[c]

        fine_stage(k, finish)
        begin(to, (2, 3))

    arriving[0].wait()
    arriving[1].wait()
    pl.semaphore_wait(barrier, sum(jnp.where(has, 1, 0) for _, _, has in ways + tuple(corners)))
    for p in range(PIECES):
        for side in (0, 1):
            leave_edge(0, side, p, [first[c, 1 + (X - 1) * side, pl.ds(p * H, H)] for c in range(3)])
    for i in range(X):
        for c in range(3):
            edge_rows(0, X, c, i, first[c, i + 1])
        edge_rows(0, X, 3, i, heat[i])
    begin(0, (2, 3))
    for copy in arriving[2:]:
        copy.wait()
    for i in range(X):
        put(inv1, i, inverse(layer(stiff, i, 6)))
        obst1[i] = jnp.where(touch[i] == 1, clear[i], FREE)
    arrive(0, (2, 3))
    for i in range(X):
        h = heat[i]
        along = load[0, i]
        if i > 0:
            along = along + heat[i - 1]
        if i < X - 1:
            along = along - heat[i + 1]
        force[0, i] = along
        force[1, i] = load[1, i] - (below(0, X, 3, i, h, 1) - above(0, X, 3, i, h, 1))
        force[2, i] = load[2, i] - (after(h, 1) - before(h, 1))

    fine_sweep(0, 1)
    for j in range(X2):
        k = [0.125 * group(stiff[c, 2 * j], stiff[c, 2 * j + 1], 1, plus) for c in range(6)]
        put(k2, j, k)
        put(inv2, j, inverse(k))
        for side, end in ((0, 0), (1, X2 - 1)):
            if j == end:
                xs[4, side, 0] = pack(k[0:4])
                xs[4, side, 1] = pack([k[4], k[5], k[5]])
        for c in range(6):
            edge_rows(4, X2, c, j, k[c])
    begin(4)
    fine_sweep(1, 2)
    arrive(4, (0, 1, 2, 3))
    for side in (0, 1):
        k = unpack(xr[4, side, 0], True) + unpack(xr[4, side, 1])[0:2]
        for c, x in enumerate(k + inverse(k)):
            halo_x[side, c] = x
        for j in range(X2):
            k = [
                jnp.broadcast_to(yr[4, side, c * X2 + j : c * X2 + j + 1, :], (8, Z))
                for c in range(6)
            ]
            for c, x in enumerate(k + inverse(k)):
                halo_y[side, j, c] = x
    for j in range(X3):
        k = [0.125 * group(k2[c, 2 * j], k2[c, 2 * j + 1], 2, plus) for c in range(6)]
        put(k3, j, k)
        put(inv3, j, inverse(k))
    for j in range(X2):
        gaps = []
        for i in (2 * j, 2 * j + 1):
            allowed = (touch[i] == 1) & (clip[i] == 0)
            gaps.append(jnp.where(allowed, clear[i] - fine_ref(2)[0, i + 1], FREE))
        obst2[j] = group(gaps[0], gaps[1], 1, jnp.minimum)

    def coarse_store(k, layers, m, j, v):
        for side, end in ((0, 0), (1, layers - 1)):
            if j == end:
                xs[k, side, 0] = pack(v)
        put(m, j, v)
        for c in range(3):
            edge_rows(k, layers, c, j, v[c])
        for side, end in ((0, 0), (1, layers - 1)):
            if j == end:
                begin(k, (side,))

    def coarse_stage(k, layers, s, m, blocks, right, finish):
        stage(
            k,
            layers,
            s,
            lambda j: layer(m, j),
            lambda j: layer(blocks, j, 6),
            lambda j: layer(right, j),
            lambda side: unpack(xr[k, side, 0]),
            finish,
        )

    def twice_begin(k, m):
        for side, near, far in ((0, 0, 1), (1, X2 - 1, X2 - 2)):
            xs[k, side, 0] = pack(layer(m, near))
            xs[k, side, 1] = pack(layer(m, far))
            if k == 3:
                xs[k, side, 2] = pack(layer(g2, near) + [obst2[near]])
            begin(k, (side,))
        for p, end in ((0, 0), (1, X2 - 1)):
            for q, at in ((0, 0), (1, Y - 1)):
                for c in range(3):
                    ds[TWICE.index(k), 2 * p + q, c : c + 1, :] = m[c, end, at : at + 1, :]
        cross_all(k, "begin")
        for j in range(X2):
            v = layer(m, j)
            rows = v + [None] * 3
            if k == 3:
                rows = rows + layer(g2, j) + [obst2[j]]
            for n, x in enumerate(rows):
                if x is not None:
                    edge_rows(k, X2, n, j, x)
            for c in range(3):
                n = (3 + c) * X2 + j
                ys[k, 0, n : n + 1, :] = v[c][2:3, :]
                ys[k, 1, n : n + 1, :] = v[c][Y - 3 : Y - 2, :]
        begin(k, (2, 3))

    def twice(k, m, keep, finish):
        def spill(side, n, j):
            return yr[k, side, n * X2 + j : n * X2 + j + 1, :]

        def wide(x):
            return jnp.broadcast_to(x, (8, Z))

        def rest_at(v, low, high, top, bottom, blocks, right):
            kv = symmetric_times(blocks, v)
            rest = []
            for c in range(3):
                if v[c].shape[0] == 8:
                    rise, fall = top[c], bottom[c]
                else:
                    rise = jnp.where(row < 2, top[c], pltpu.roll(v[c], 2, 0))
                    fall = jnp.where(row >= Y - 2, bottom[c], pltpu.roll(v[c], Y - 2, 0))
                near = (low[c] + high[c]) + (rise + fall) + (before(v[c], 2) + after(v[c], 2))
                rest.append(right[c] - kv[c] + near)
            return rest

        own = [layer(m, j) for j in range(X2)]
        arrive(k, (2, 3))
        arrive(k, (0, 1))
        cross_all(k, "arrive")
        xh = [[unpack(xr[k, side, n]) for n in (0, 1)] for side in (0, 1)]
        ext = [xh[0][0]] + own + [xh[1][0]]
        done = [None] * (X2 + 2)
        for j in range(X2):
            top, bottom = ([spill(side, c, j) for c in range(3)] for side in (0, 1))
            rest = rest_at(own[j], ext[j], ext[j + 2], top, bottom, layer(k2, j, 6), layer(g2, j))
            done[j + 1] = relaxed(own[j], layer(inv2, j, 6), rest, obst2[j])
            put(keep, j, done[j + 1])

        def corner(p, q):
            return [dr[TWICE.index(k), 2 * p + q, c : c + 1, :] for c in range(3)]

        for side in (0, 1):
            if k == 3:
                for c, x in enumerate(unpack(xr[3, side, 2], True)):
                    halo_x[side, 12 + c] = x
            st = [halo_x[side, c] for c in range(16)]
            inner = own[0] if side == 0 else own[X2 - 1]
            v = xh[side][0]
            rest = rest_at(v, xh[side][1], inner, corner(side, 0), corner(side, 1), st, st[12:15])
            w = relaxed(v, st[6:12], rest, st[15])
            done[(X2 + 1) * side] = [jnp.where(ways[side][2], x, 0.0) for x in w]
        rims = []
        for side in (0, 1):
            line = [[wide(spill(side, c, j)) for c in range(3)] for j in range(X2)]
            line = [[wide(x) for x in corner(0, side)]] + line
            line = line + [[wide(x) for x in corner(1, side)]]
            rims.append([])
            for j in range(X2):
                st = [halo_y[side, j, c] for c in range(12)]
                st = st + [wide(yr[3, side, n * X2 + j : n * X2 + j + 1, :]) for n in range(6, 10)]
                far = [wide(spill(side, 3 + c, j)) for c in range(3)]
                at = 0 if side == 0 else Y - 1
                inner = [wide(m[c, j, at : at + 1, :]) for c in range(3)]
                v = line[j + 1]
                rest = rest_at(v, line[j], line[j + 2], far, inner, st, st[12:15])
                w = relaxed(v, st[6:12], rest, st[15])
                rims[side].append([jnp.where(ways[2 + side][2], x, 0.0)[0:1, :] for x in w])
        for j in range(X2):
            rest = rest_at(
                done[j + 1], done[j], done[j + 2], rims[0][j], rims[1][j],
                layer(k2, j, 6), layer(g2, j),
            )
            finish(j, done[j + 1], rest)

    m0, m1, m2, m3, m4 = (middle.at[n] for n in range(5))
    fine_rests = {}

    def restrict(i, p, rest):
        fine_rests[i, p] = [jnp.where(clip[i, pl.ds(p * H, H)] == 1, 0.0, rest[0]), rest[1], rest[2]]
        j = i // 2
        if all((n, q) in fine_rests for n in (2 * j, 2 * j + 1) for q in range(PIECES)):
            pair = [
                [jnp.concatenate([fine_rests[n, q][c] for q in range(PIECES)], 0) for c in range(3)]
                for n in (2 * j, 2 * j + 1)
            ]
            right = [0.25 * group(pair[0][c], pair[1][c], 1, plus) for c in range(3)]
            put(g2, j, right)
            put(m0, j, opened(layer(inv2, j, 6), right, obst2[j]))

    fine_stage(2, restrict)
    twice_begin(3, m0)

    middle_rests = {}

    def restrict_again(i, v, rest):
        middle_rests[i] = rest
        j = i // 2
        if 2 * j in middle_rests and 2 * j + 1 in middle_rests:
            pair = middle_rests[2 * j], middle_rests[2 * j + 1]
            right = [0.25 * group(pair[0][c], pair[1][c], 2, plus) for c in range(3)]
            gaps = [obst2[n] - m1[0, n] for n in (2 * j, 2 * j + 1)]
            obst3[j] = group(gaps[0], gaps[1], 2, jnp.minimum)
            put(g3, j, right)
            coarse_store(5, X3, m4, j, opened(layer(inv3, j, 6), right, obst3[j]))

    twice(3, m0, m1, restrict_again)
    begin(5, (2, 3))

    def lowest(j, v, rest):
        low = relaxed(v, layer(inv3, j, 6), rest, obst3[j])
        for n in (2 * j, 2 * j + 1):
            put(m2, n, [m1[c, n] + low[c] for c in range(3)])

    coarse_stage(5, X3, 4, m4, k3, g3, lowest)
    twice_begin(6, m2)

    def raise_back(j, v, rest):
        w = relaxed(v, layer(inv2, j, 6), rest, obst2[j])
        for i in (2 * j, 2 * j + 1) if j < X2 - 1 else (2 * j + 1, 2 * j):
            old = layer(fine_ref(2), i + 1)
            w0 = jnp.where(clip[i] == 1, 0.0, w[0])
            new = [old[0] + w0, old[1] + w[1], old[2] + w[2]]
            for p in range(PIECES):
                fine_store(8, i, p, [x[p * H : p * H + H] for x in new])

    twice(6, m2, m3, raise_back)
    begin(8, (2, 3))
    fine_sweep(8, 9)
    fine_sweep(9, 10)

    def remain(i, p, rest):
        for c in range(3):
            resid[c, i, pl.ds(p * H, H)] = rest[c]

    fine_stage(10, remain)
    for k in USED:
        leave(k)
    for k in TWICE:
        cross_all(k, "leave")


def local(*args):
    disp, _, heat = args[:3]
    X, Y, Z = heat.shape
    X2, X3 = X // 2, X // 4
    f32 = jnp.float32

    def buffer(*shape, dtype=f32):
        return pltpu.VMEM(shape + (Y, Z), dtype)

    rows = -(-5 * X // 8) * 8
    scratch = [
        buffer(3, X + 2),
        buffer(X),
        buffer(5, 3, X + 2),
        buffer(len(FINE), 2, 3),
        buffer(5, 3, X2),
        buffer(EXCHANGES, 2, 3),
        buffer(EXCHANGES, 2, 3),
        pltpu.VMEM((EXCHANGES, 2, rows, Z), f32),
        pltpu.VMEM((EXCHANGES, 2, rows, Z), f32),
        pltpu.VMEM((2, 4, 8, Z), f32),
        pltpu.VMEM((2, 4, 8, Z), f32),
        buffer(2, 16),
        pltpu.VMEM((2, X2, 12, 8, Z), f32),
        buffer(3, X),
        buffer(6, X),
        buffer(X),
        buffer(X, dtype=jnp.int32),
        buffer(X, dtype=jnp.int32),
        buffer(3, X),
        buffer(3, X),
        buffer(6, X),
        buffer(X),
        buffer(3, X2),
        buffer(6, X2),
        buffer(6, X2),
        buffer(X2),
        buffer(3, X3),
        buffer(6, X3),
        buffer(6, X3),
        buffer(X3),
        pltpu.SemaphoreType.DMA((8,)),
        pltpu.SemaphoreType.DMA((EXCHANGES, 4, PIECES)),
        pltpu.SemaphoreType.DMA((EXCHANGES, 4, PIECES)),
        pltpu.SemaphoreType.DMA((2, 4)),
        pltpu.SemaphoreType.DMA((2, 4)),
    ]
    anywhere = pl.BlockSpec(memory_space=pl.ANY)
    return pl.pallas_call(
        kernel,
        out_shape=[pltpu.VMEM(disp.shape, f32)] * 2,
        in_specs=[anywhere] * 8,
        out_specs=[pl.BlockSpec(memory_space=pltpu.VMEM)] * 2,
        scratch_shapes=scratch,
        compiler_params=pltpu.CompilerParams(collective_id=0, has_side_effects=True),
        name="vcycle",
    )(*args)


def solution(mesh):
    whole = P(None, "grp", "brick", None)
    flat = P("grp", "brick", None)
    return jax.shard_map(
        local,
        mesh=mesh,
        in_specs=(whole, whole, flat, whole, whole, flat, flat, flat),
        out_specs=(whole, whole),
        check_vma=False,
    )
```

```python
import jax
import jax.numpy as jnp
from jax import lax
from jax.experimental import pallas as pl
from jax.experimental.pallas import tpu as pltpu
from jax.sharding import PartitionSpec as P

OMEGA = 0.6
FREE = 1000.0
FINE = (0, 1, 2, 8, 9, 10)
PIECES = 2
RING = 2
AROUND = [(1, 0), (-1, 0), (1, 1), (1, -1), (-1, 1), (-1, -1), (2, 0), (-2, 0)]
AROUND += [(0, 1), (0, -1), (2, 1), (2, -1), (-2, 1), (-2, -1)]
STRAIGHT = [n for n, (di, dj) in enumerate(AROUND) if not (di and dj)]
DIAGONAL = [n for n, (di, dj) in enumerate(AROUND) if di and dj]
NEXT = [n for n, (di, dj) in enumerate(AROUND) if abs(di) < 2]
OPPOSITE = [AROUND.index((-di, -dj)) for di, dj in AROUND]
BLOCKS, RIGHTS = 0, 1
MESH = pl.DeviceIdType.MESH


def inverse(k, keep=None):
    a, b, c, d, e, f = k
    i00 = b * c - e * e
    i11 = a * c - f * f
    i22 = a * b - d * d
    i01 = f * e - d * c
    i12 = d * f - a * e
    i02 = d * e - b * f
    scale = 1.0 / (a * i00 + d * i01 + f * i02)
    if keep is not None:
        scale = scale * keep
    return [i00 * scale, i11 * scale, i22 * scale, i01 * scale, i12 * scale, i02 * scale]


def symmetric_times(m, v):
    return [
        m[0] * v[0] + m[3] * v[1] + m[5] * v[2],
        m[3] * v[0] + m[1] * v[1] + m[4] * v[2],
        m[5] * v[0] + m[4] * v[1] + m[2] * v[2],
    ]


def kernel(
    disp_h, load_h, heat_h, diag_h, off_h, clear_h, touch_h, clip_h,
    moved, resid,
    first, heat, fine, edge, ys, yr, load, stiff, clear, touch, clip,
    force, rests, inv1, obst1,
    squeezed, kring, gring, iring, ksend, kfrom, gsend, gfrom, m0, m1, m2, m3, inv3, m4, low,
    in_sem, send_sem, recv_sem, ring_send, ring_recv, low_send, low_recv,
):
    X, Y, Z = heat_h.shape
    X2, X3 = X // 2, X // 4
    H = Y // PIECES
    h, w = Y // 2, Z // 2
    g, b = lax.axis_index("grp"), lax.axis_index("brick")
    ng, nb = lax.axis_size("grp"), lax.axis_size("brick")
    ways = (
        ("grp", g - 1, g > 0),
        ("grp", g + 1, g < ng - 1),
        ("brick", b - 1, b > 0),
        ("brick", b + 1, b < nb - 1),
    )
    barrier = pltpu.get_barrier_semaphore()
    for axis, there, has in ways:

        @pl.when(has)
        def _():
            pl.semaphore_signal(barrier, inc=1, device_id={axis: there}, device_id_type=MESH)

    def reaches(di, dj):
        has = None
        for d, at, count in ((di, g, ng), (dj, b, nb)):
            if d:
                inside = at + d >= 0 if d < 0 else at + d < count
                has = inside if has is None else has & inside
        return has

    around = [reaches(di, dj) for di, dj in AROUND]
    for (di, dj), has in zip(AROUND, around):
        if abs(di) + abs(dj) > 1:

            @pl.when(has)
            def _():
                pl.semaphore_signal(
                    barrier, inc=1, device_id={"grp": g + di, "brick": b + dj}, device_id_type=MESH
                )

    pairs = (
        (disp_h, first.at[:, 1 : X + 1]),
        (heat_h, heat),
        (diag_h, stiff.at[0:3]),
        (off_h, stiff.at[3:6]),
        (load_h, load),
        (clear_h, clear),
        (touch_h, touch),
        (clip_h, clip),
    )
    arriving = [pltpu.make_async_copy(s, d, in_sem.at[i]) for i, (s, d) in enumerate(pairs)]
    for copy in arriving:
        copy.start()

    row = lax.broadcasted_iota(jnp.int32, (Y, Z), 0)
    lane = lax.broadcasted_iota(jnp.int32, (Y, Z), 1)
    crow = lax.broadcasted_iota(jnp.int32, (h, w), 0)
    clane = lax.broadcasted_iota(jnp.int32, (h, w), 1)
    slane = lax.broadcasted_iota(jnp.int32, (Y, w), 1)
    own, mid = pl.ds(RING * X2, X2), pl.ds(h, h)

    def fine_ref(k):
        return first if k == 0 else fine.at[FINE.index(k) - 1]

    for way, (axis, there, has) in enumerate(ways):

        @pl.when(jnp.logical_not(has))
        def _():
            for k in FINE:
                if way >= 2:
                    yr[FINE.index(k), way - 2] = jnp.zeros(yr.shape[2:], jnp.float32)
                else:
                    for c in range(3):
                        fine_ref(k)[c, 0 if way == 0 else X + 1] = jnp.zeros((Y, Z), jnp.float32)

    for n, (di, dj) in enumerate(AROUND):

        @pl.when(jnp.logical_not(around[n]))
        def _():
            for ref, fill in ((kring, (1.0,) * 3 + (0.0,) * 3), (gring, (0.0,) * 3 + (FREE,))):
                for c, x in enumerate(fill):
                    if n in DIAGONAL:
                        spot = kfrom if ref is kring else gfrom
                        spot[DIAGONAL.index(n), c] = jnp.full((h, w), x, jnp.float32)
                    else:
                        for j in range(X2):
                            ref[c, (di + RING) * X2 + j, pl.ds((dj + 1) * h, h)] = jnp.full((h, w), x, jnp.float32)
            if n in NEXT:
                for c in range(3):
                    low[c, di + 1, pl.ds((dj + 1) * h, h)] = jnp.zeros((h, w), jnp.float32)

    def transfer(k, way, p=0):
        m = FINE.index(k)
        if way >= 2:
            src, dst = ys.at[m, way - 2], yr.at[m, 3 - way]
        else:
            part = pl.ds(p * H, H)
            src = edge.at[m, way, :, part]
            dst = fine_ref(k).at[:, 0 if way else X + 1, part]
        axis, there, _ = ways[way]
        return pltpu.make_async_remote_copy(
            src_ref=src,
            dst_ref=dst,
            send_sem=send_sem.at[m, way, p],
            recv_sem=recv_sem.at[m, way ^ 1, p],
            device_id={axis: there},
            device_id_type=MESH,
        )

    def begin(k, sides=(0, 1, 2, 3), p=0):
        for way in sides:

            @pl.when(ways[way][2])
            def _():
                transfer(k, way, p).start()

    def arrive(k, sides, p=0):
        for side in sides:

            @pl.when(ways[side][2])
            def _():
                transfer(k, side ^ 1, p).wait_recv()

    def leave(k):
        for way in range(4):

            @pl.when(ways[way][2])
            def _():
                for p in range(PIECES if way < 2 else 1):
                    transfer(k, way, p).wait_send()

    def ring_copy(kind, n):
        di, dj = AROUND[n]
        m = OPPOSITE[n]
        if n in DIAGONAL:
            src = (ksend, gsend)[kind].at[0 if dj < 0 else 1]
            dst = (kfrom, gfrom)[kind].at[DIAGONAL.index(m)]
        else:
            ref = (kring, gring)[kind]
            src = ref.at[:, own, mid]
            dst = ref.at[:, pl.ds((RING - di) * X2, X2), pl.ds((1 - dj) * h, h)]
        return pltpu.make_async_remote_copy(
            src_ref=src,
            dst_ref=dst,
            send_sem=ring_send.at[kind, n],
            recv_sem=ring_recv.at[kind, m],
            device_id={"grp": g + di, "brick": b + dj},
            device_id_type=MESH,
        )

    def low_copy(n):
        di, dj = AROUND[n]
        return pltpu.make_async_remote_copy(
            src_ref=low.at[:, 1, mid],
            dst_ref=low.at[:, 1 - di, pl.ds((1 - dj) * h, h)],
            send_sem=low_send.at[n],
            recv_sem=low_recv.at[OPPOSITE[n]],
            device_id={"grp": g + di, "brick": b + dj},
            device_id_type=MESH,
        )

    def ring_begin(copy, which):
        for n in which:

            @pl.when(around[n])
            def _():
                copy(n).start()

    def ring_arrive(copy, which):
        for n in which:

            @pl.when(around[n])
            def _():
                copy(OPPOSITE[n]).wait_recv()

    def ring_leave(copy, which):
        for n in which:

            @pl.when(around[n])
            def _():
                copy(n).wait_send()

    def corners_pack(ref, out, count):
        for c in range(count):
            near, far = ref[c, RING * X2, mid], ref[c, RING * X2 + X2 - 1, mid]
            out[0, c] = jnp.where(crow < h // 2, near, pltpu.roll(far, h // 2, 0))
            out[1, c] = jnp.where(crow < h // 2, pltpu.roll(near, h // 2, 0), far)

    def corners_unpack(out, ref, count):
        for d, n in enumerate(DIAGONAL):
            di, dj = AROUND[n]
            rows = pl.ds((dj + 1) * h, h)
            for c in range(count):
                x = out[d, c]
                y = pltpu.roll(x, h // 2, 0)
                ref[c, (di + RING) * X2, rows] = y if dj < 0 else x
                ref[c, (di + RING) * X2 + X2 - 1, rows] = x if dj < 0 else y

    def edge_rows(k, layers, c, i, v):
        n = c * layers + i
        m = FINE.index(k)
        ys[m, 0, n : n + 1, :] = v[0:1, :]
        ys[m, 1, n : n + 1, :] = v[Y - 1 : Y, :]

    def before(v, s):
        at = lane if v.shape[1] == Z else clane
        return jnp.where(at < s, 0.0, pltpu.roll(v, s, 1))

    def after(v, s):
        at = lane if v.shape[1] == Z else clane
        size = v.shape[1]
        return jnp.where(at >= size - s, 0.0, pltpu.roll(v, size - s, 1))

    def above(k, layers, c, i, v, s):
        n = c * layers + i
        return jnp.where(row < s, yr[FINE.index(k), 0, n : n + 1, :], pltpu.roll(v, s, 0))

    def below(k, layers, c, i, v, s):
        n = c * layers + i
        return jnp.where(row >= Y - s, yr[FINE.index(k), 1, n : n + 1, :], pltpu.roll(v, Y - s, 0))

    def shrink(slot, v, how):
        v = how(v, pltpu.roll(v, Z - 1, 1))
        spots = (2 * slane) & (w - 1)
        lo = jnp.take_along_axis(v[:, 0:w], spots, axis=1)
        hi = jnp.take_along_axis(v[:, w:Z], spots, axis=1)
        squeezed[slot] = jnp.where(slane < w // 2, lo, hi)
        return how(squeezed[slot, pl.ds(0, h, stride=2), :], squeezed[slot, pl.ds(1, h, stride=2), :])

    def grow(slot, x):
        squeezed[slot, pl.ds(0, h, stride=2), :] = x
        squeezed[slot, pl.ds(1, h, stride=2), :] = x
        v = squeezed[slot]
        spots = slane >> 1
        parts = [jnp.take_along_axis(v, spots + n * (w // 2), axis=1) for n in (0, 1)]
        return jnp.concatenate(parts, 1)

    def pair(v, axis, how):
        size = v.shape[axis]
        at = (crow, clane)[axis]
        return how(v, jnp.where((at & 1) == 0, pltpu.roll(v, size - 1, axis), pltpu.roll(v, 1, axis)))

    def group(v, w, how):
        return pair(pair(how(v, w), 1, how), 0, how)

    def plus(v, w):
        return v + w

    def layer(ref, i, count=3):
        return [ref[c, i] for c in range(count)]

    def put(ref, i, values):
        for c, v in enumerate(values):
            ref[c, i] = v

    def relaxed(v, inv, rest, obstacle):
        step = symmetric_times(inv, rest)
        w = [v[c] + OMEGA * step[c] for c in range(3)]
        return [jnp.minimum(w[0], obstacle), w[1], w[2]]

    def opened(inv, right, obstacle):
        w = [OMEGA * x for x in symmetric_times(inv, right)]
        return [jnp.minimum(w[0], obstacle), w[1], w[2]]

    def fine_stage(k, finish):
        ref, m = fine_ref(k), FINE.index(k)
        for i in range(X):
            v = layer(ref, i + 1)
            kv = symmetric_times(layer(stiff, i, 6), v)
            for c in range(3):
                near = jnp.where(row < 1, 0.0, pltpu.roll(v[c], 1, 0))
                near = near + jnp.where(row >= Y - 1, 0.0, pltpu.roll(v[c], Y - 1, 0))
                near = near + (before(v[c], 1) + after(v[c], 1))
                r = (force[c, i] - kv[c]) + near
                for n in (i - 1, i + 1):
                    if 0 <= n < X:
                        r = r + ref[c, n + 1]
                rests[c, i] = r
        if k > 0:
            arrive(k, (2, 3))
        for i in range(X):
            for c in range(3):
                n = c * X + i
                rests[c, i, 0:1, :] = rests[c, i, 0:1, :] + yr[m, 0, n : n + 1, :]
                rests[c, i, Y - 1 : Y, :] = rests[c, i, Y - 1 : Y, :] + yr[m, 1, n : n + 1, :]
        for i in range(1, X - 1):
            for p in range(PIECES):
                finish(i, p, [rests[c, i, pl.ds(p * H, H)] for c in range(3)])
        for p in range(PIECES):
            part = pl.ds(p * H, H)
            for side, i in ((0, 0), (1, X - 1)):
                arrive(k, (side,), p)
                rest = [rests[c, i, part] + ref[c, (X + 1) * side, part] for c in range(3)]
                if X == 1 and side == 0:
                    for c in range(3):
                        rests[c, i, part] = rest[c]
                else:
                    finish(i, p, rest)

    def leave_edge(k, side, p, w):
        part = pl.ds(p * H, H)
        h = heat[(X - 1) * side, part]
        edge[FINE.index(k), side, 0, part] = w[0] + h if side else w[0] - h
        for c in (1, 2):
            edge[FINE.index(k), side, c, part] = w[c]
        begin(k, (side,), p)

    def fine_store(to, i, p, w):
        for c in range(3):
            fine_ref(to)[c, i + 1, pl.ds(p * H, H)] = w[c]
        for side, end in ((0, 0), (1, X - 1)):
            if i == end:
                leave_edge(to, side, p, w)
        for c in range(3):
            n = c * X + i
            if p == 0:
                ys[FINE.index(to), 0, n : n + 1, :] = w[c][0:1, :]
            if p == PIECES - 1:
                ys[FINE.index(to), 1, n : n + 1, :] = w[c][H - 1 : H, :]

    def fine_sweep(k, to):
        def finish(i, p, rest):
            part = pl.ds(p * H, H)
            v = [fine_ref(k)[c, i + 1, part] for c in range(3)]
            w = relaxed(v, [inv1[c, i, part] for c in range(6)], rest, obst1[i, part])
            fine_store(to, i, p, w)
            if to == 10:
                for c in range(3):
                    moved[c, i, part] = w[c]

        fine_stage(k, finish)
        begin(to, (2, 3))

    arriving[0].wait()
    arriving[1].wait()
    pl.semaphore_wait(barrier, sum(jnp.where(has, 1, 0) for has in around))
    for p in range(PIECES):
        for side in (0, 1):
            leave_edge(0, side, p, [first[c, 1 + (X - 1) * side, pl.ds(p * H, H)] for c in range(3)])
    for i in range(X):
        for c in range(3):
            edge_rows(0, X, c, i, first[c, i + 1])
        edge_rows(0, X, 3, i, heat[i])
    begin(0, (2, 3))
    for copy in arriving[2:]:
        copy.wait()
    for i in range(X):
        put(inv1, i, inverse(layer(stiff, i, 6)))
        obst1[i] = jnp.where(touch[i] == 1, clear[i], FREE)
    arrive(0, (2, 3))
    for i in range(X):
        warm = heat[i]
        along = load[0, i]
        if i > 0:
            along = along + heat[i - 1]
        if i < X - 1:
            along = along - heat[i + 1]
        force[0, i] = along
        force[1, i] = load[1, i] - (below(0, X, 3, i, warm, 1) - above(0, X, 3, i, warm, 1))
        force[2, i] = load[2, i] - (after(warm, 1) - before(warm, 1))

    for j in range(X2):
        for c in range(6):
            both = stiff[c, 2 * j] + stiff[c, 2 * j + 1]
            kring[c, RING * X2 + j, mid] = 0.125 * shrink(6 * j + c, both, plus)
    blocks_copy, rights_copy = (lambda n: ring_copy(BLOCKS, n)), (lambda n: ring_copy(RIGHTS, n))
    ring_begin(blocks_copy, STRAIGHT)
    fine_sweep(0, 1)
    corners_pack(kring, ksend, 6)
    ring_begin(blocks_copy, DIAGONAL)
    fine_sweep(1, 2)

    def block(ref, i, t, count=3):
        return [ref[c, i, t * h : t * h + h, :] for c in range(count)]

    def block_put(ref, i, t, values):
        for c, x in enumerate(values):
            ref[c, i, t * h : t * h + h, :] = x

    first_own = RING * X2
    last_own = first_own + X2 - 1

    def region(straight, sideways):
        spots = [(i, 1) for i in range(first_own - straight, last_own + straight + 1)]
        for t in (0, 2):
            spots += [(i, t) for i in range(first_own - sideways, last_own + sideways + 1)]
        return spots

    def keep(di, dj):
        if (di, dj) == (0, 0):
            return None
        return jnp.where(around[AROUND.index((di, dj))], 1.0, 0.0)

    for j in range(X2):
        gaps = []
        for i in (2 * j, 2 * j + 1):
            allowed = (touch[i] == 1) & (clip[i] == 0)
            gaps.append(jnp.where(allowed, clear[i] - fine_ref(2)[0, i + 1], FREE))
        gring[3, first_own + j, mid] = shrink(j, jnp.minimum(gaps[0], gaps[1]), jnp.minimum)
    ring_arrive(blocks_copy, range(len(AROUND)))
    corners_unpack(kfrom, kring, 6)
    for i, t in region(4, 3):
        block_put(iring, i, t, inverse(block(kring, i, t, 6), keep(i // X2 - RING, t - 1)))
    thirds = [(0, 1), (1, 1), (2, 1), (1, 0), (1, 2)]
    base = first_own - 2
    k3 = None
    for n, (q, t) in enumerate(thirds):
        pairs = [block(kring, base + 2 * q + e, t, 6) for e in (0, 1)]
        k = [0.125 * group(pairs[0][c], pairs[1][c], plus) for c in range(6)]
        if (q, t) == (1, 1):
            k3 = k
        for c, x in enumerate(inverse(k, keep(q - 1, t - 1))):
            inv3[n, c] = x
    for c in range(6):
        inv3[len(thirds), c] = k3[c]

    fine_rests = {}

    def restrict(i, p, rest):
        fine_rests[i, p] = [jnp.where(clip[i, pl.ds(p * H, H)] == 1, 0.0, rest[0]), rest[1], rest[2]]
        j = i // 2
        if all((n, q) in fine_rests for n in (2 * j, 2 * j + 1) for q in range(PIECES)):
            for c in range(3):
                both = [fine_rests[2 * j, q][c] + fine_rests[2 * j + 1, q][c] for q in range(PIECES)]
                right = 0.25 * shrink(X2 + 3 * j + c, jnp.concatenate(both, 0), plus)
                gring[c, first_own + j, mid] = right

    fine_stage(2, restrict)
    ring_begin(rights_copy, [n for n in STRAIGHT if abs(AROUND[n][0]) == 1])
    corners_pack(gring, gsend, 4)
    ring_begin(rights_copy, DIAGONAL)
    ring_begin(rights_copy, [n for n in STRAIGHT if abs(AROUND[n][0]) != 1])
    ring_arrive(rights_copy, range(len(AROUND)))
    corners_unpack(gfrom, gring, 4)

    def ring_rest(m, i, t):
        v = block(m, i, t)
        kv = symmetric_times(block(kring, i, t, 6), v)
        right = block(gring, i, t)
        rest = []
        for c in range(3):
            up = m[c, i, t * h - 1 : t * h + h - 1, :] if t > 0 else pltpu.roll(v[c], 1, 0)
            down = m[c, i, t * h + 1 : t * h + h + 1, :] if t < 2 else pltpu.roll(v[c], h - 1, 0)
            near = (up + down) + (before(v[c], 1) + after(v[c], 1))
            near = near + (m[c, i - 1, t * h : t * h + h, :] + m[c, i + 1, t * h : t * h + h, :])
            rest.append((right[c] - kv[c]) + near)
        return rest

    def ring_sweep(m, i, t):
        obstacle = gring[3, i, t * h : t * h + h, :]
        return relaxed(block(m, i, t), block(iring, i, t, 6), ring_rest(m, i, t), obstacle)

    for i, t in region(4, 3):
        obstacle = gring[3, i, t * h : t * h + h, :]
        block_put(m0, i, t, opened(block(iring, i, t, 6), block(gring, i, t), obstacle))
    for i, t in region(3, 2):
        block_put(m1, i, t, ring_sweep(m0, i, t))
    g3 = obst3 = None
    for n, (q, t) in enumerate(thirds):
        spots = (base + 2 * q, base + 2 * q + 1)
        rest = [ring_rest(m1, i, t) for i in spots]
        right = [0.25 * group(rest[0][c], rest[1][c], plus) for c in range(3)]
        gaps = [gring[3, i, t * h : t * h + h, :] - m1[0, i, t * h : t * h + h, :] for i in spots]
        obstacle = group(gaps[0], gaps[1], jnp.minimum)
        if (q, t) == (1, 1):
            g3, obst3 = right, obstacle
        block_put(m4, q, t, opened([inv3[n, c] for c in range(6)], right, obstacle))
    v = block(m4, 1, 1)
    kv = symmetric_times([inv3[len(thirds), c] for c in range(6)], v)
    rest = []
    for c in range(3):
        near = m4[c, 1, h - 2 : 2 * h - 2, :] + m4[c, 1, h + 2 : 2 * h + 2, :]
        near = near + (before(v[c], 2) + after(v[c], 2)) + (m4[c, 0, h : 2 * h, :] + m4[c, 2, h : 2 * h, :])
        rest.append((g3[c] - kv[c]) + near)
    block_put(low, 1, 1, relaxed(v, [inv3[1, c] for c in range(6)], rest, obst3))
    ring_begin(low_copy, NEXT)
    ring_arrive(low_copy, NEXT)
    for i, t in region(2, 1):
        lows = block(low, (i - base) // 2, t)
        block_put(m2, i, t, [x + y for x, y in zip(block(m1, i, t), lows)])
    for i, t in region(1, 0):
        block_put(m3, i, t, ring_sweep(m2, i, t))
    for j in (0, X2 - 1) if X2 > 1 else (0,):
        lift = [grow(3 * j + c, x) for c, x in enumerate(ring_sweep(m3, first_own + j, 1))]
        for i in (2 * j, 2 * j + 1) if j < X2 - 1 else (2 * j + 1, 2 * j):
            old = layer(fine_ref(2), i + 1)
            lift0 = jnp.where(clip[i] == 1, 0.0, lift[0])
            new = [old[0] + lift0, old[1] + lift[1], old[2] + lift[2]]
            for p in range(PIECES):
                fine_store(8, i, p, [x[p * H : p * H + H] for x in new])
    begin(8, (2, 3))
    fine_sweep(8, 9)
    fine_sweep(9, 10)

    def remain(i, p, rest):
        for c in range(3):
            resid[c, i, pl.ds(p * H, H)] = rest[c]

    fine_stage(10, remain)
    for k in FINE:
        leave(k)
    ring_leave(blocks_copy, range(len(AROUND)))
    ring_leave(rights_copy, range(len(AROUND)))
    ring_leave(low_copy, NEXT)


def local(*args):
    disp, _, heat = args[:3]
    X, Y, Z = heat.shape
    X2 = X // 2
    h, w = Y // 2, Z // 2
    f32 = jnp.float32

    def buffer(*shape, dtype=f32):
        return pltpu.VMEM(shape + (Y, Z), dtype)

    def small(*shape):
        return pltpu.VMEM(shape + (w,), f32)

    rows = -(-4 * X // 8) * 8
    layers, tall, corners = (2 * RING + 1) * X2, 3 * h, len(DIAGONAL)
    scratch = [
        buffer(3, X + 2),
        buffer(X),
        buffer(5, 3, X + 2),
        buffer(len(FINE), 2, 3),
        pltpu.VMEM((len(FINE), 2, rows, Z), f32),
        pltpu.VMEM((len(FINE), 2, rows, Z), f32),
        buffer(3, X),
        buffer(6, X),
        buffer(X),
        buffer(X, dtype=jnp.int32),
        buffer(X, dtype=jnp.int32),
        buffer(3, X),
        buffer(3, X),
        buffer(6, X),
        buffer(X),
        small(6 * X2, Y),
        small(6, layers, tall),
        small(4, layers, tall),
        small(6, layers, tall),
        small(2, 6, h),
        small(corners, 6, h),
        small(2, 4, h),
        small(corners, 4, h),
        small(3, layers, tall),
        small(3, layers, tall),
        small(3, layers, tall),
        small(3, layers, tall),
        small(6, 6, h),
        small(3, 3, tall),
        small(3, 3, tall),
        pltpu.SemaphoreType.DMA((8,)),
        pltpu.SemaphoreType.DMA((len(FINE), 4, PIECES)),
        pltpu.SemaphoreType.DMA((len(FINE), 4, PIECES)),
        pltpu.SemaphoreType.DMA((2, len(AROUND))),
        pltpu.SemaphoreType.DMA((2, len(AROUND))),
        pltpu.SemaphoreType.DMA((len(AROUND),)),
        pltpu.SemaphoreType.DMA((len(AROUND),)),
    ]
    anywhere = pl.BlockSpec(memory_space=pl.ANY)
    return pl.pallas_call(
        kernel,
        out_shape=[pltpu.VMEM(disp.shape, f32)] * 2,
        in_specs=[anywhere] * 8,
        out_specs=[pl.BlockSpec(memory_space=pltpu.VMEM)] * 2,
        scratch_shapes=scratch,
        compiler_params=pltpu.CompilerParams(collective_id=0, has_side_effects=True),
        name="vcycle",
    )(*args)


def solution(mesh):
    whole = P(None, "grp", "brick", None)
    flat = P("grp", "brick", None)
    return jax.shard_map(
        local,
        mesh=mesh,
        in_specs=(whole, whole, flat, whole, whole, flat, flat, flat),
        out_specs=(whole, whole),
        check_vma=False,
    )
```

```python
import jax
import jax.numpy as jnp
from jax import lax
from jax.experimental import pallas as pl
from jax.experimental.pallas import tpu as pltpu
from jax.sharding import PartitionSpec as P

OMEGA = 0.6
FREE = 1000.0
FINE = (0, 1, 2, 8, 9, 10)
PIECES = 2
RING = 2
AROUND = [(1, 0), (-1, 0), (1, 1), (1, -1), (-1, 1), (-1, -1), (2, 0), (-2, 0)]
AROUND += [(0, 1), (0, -1), (2, 1), (2, -1), (-2, 1), (-2, -1)]
STRAIGHT = [n for n, (di, dj) in enumerate(AROUND) if not (di and dj)]
DIAGONAL = [n for n, (di, dj) in enumerate(AROUND) if di and dj]
NEXT = [n for n, (di, dj) in enumerate(AROUND) if abs(di) < 2 or dj == 0]
SIDES = [AROUND.index((1, 0)), AROUND.index((-1, 0))]
CLOSE = [n for n in DIAGONAL if abs(AROUND[n][0]) == 1]
REST = [n for n in range(len(AROUND)) if n not in SIDES + CLOSE]
SENT = (0, 1, 2, 9, 10)
OPPOSITE = [AROUND.index((-di, -dj)) for di, dj in AROUND]
BLOCKS, RIGHTS, CROSS = 0, 1, 2
MESH = pl.DeviceIdType.MESH


def inverse(k, keep=None):
    a, b, c, d, e, f = k
    i00 = b * c - e * e
    i11 = a * c - f * f
    i22 = a * b - d * d
    i01 = f * e - d * c
    i12 = d * f - a * e
    i02 = d * e - b * f
    scale = 1.0 / (a * i00 + d * i01 + f * i02)
    if keep is not None:
        scale = scale * keep
    return [i00 * scale, i11 * scale, i22 * scale, i01 * scale, i12 * scale, i02 * scale]


def symmetric_times(m, v):
    return [
        m[0] * v[0] + m[3] * v[1] + m[5] * v[2],
        m[3] * v[0] + m[1] * v[1] + m[4] * v[2],
        m[5] * v[0] + m[4] * v[1] + m[2] * v[2],
    ]


def kernel(
    disp_h, load_h, heat_h, diag_h, off_h, clear_h, touch_h, clip_h,
    moved, resid,
    first, heat, fine, edge, ys, yr, load, stiff, clear, touch, clip,
    force, rests, inv1, obst1,
    squeezed, kring, gring, iring, ksend, kfrom, gsend, gfrom, m0, m1, m2, m3, inv3, m4, low,
    free, fedge, fhalo,
    in_sem, send_sem, recv_sem, ring_send, ring_recv, low_send, low_recv, free_send, free_recv,
):
    X, Y, Z = heat_h.shape
    X2, X3 = X // 2, X // 4
    H = Y // PIECES
    h, w = Y // 2, Z // 2
    g, b = lax.axis_index("grp"), lax.axis_index("brick")
    ng, nb = lax.axis_size("grp"), lax.axis_size("brick")
    ways = (
        ("grp", g - 1, g > 0),
        ("grp", g + 1, g < ng - 1),
        ("brick", b - 1, b > 0),
        ("brick", b + 1, b < nb - 1),
    )
    barrier = pltpu.get_barrier_semaphore()
    for axis, there, has in ways:

        @pl.when(has)
        def _():
            pl.semaphore_signal(barrier, inc=1, device_id={axis: there}, device_id_type=MESH)

    def reaches(di, dj):
        has = None
        for d, at, count in ((di, g, ng), (dj, b, nb)):
            if d:
                inside = at + d >= 0 if d < 0 else at + d < count
                has = inside if has is None else has & inside
        return has

    around = [reaches(di, dj) for di, dj in AROUND]
    for (di, dj), has in zip(AROUND, around):
        if abs(di) + abs(dj) > 1:

            @pl.when(has)
            def _():
                pl.semaphore_signal(
                    barrier, inc=1, device_id={"grp": g + di, "brick": b + dj}, device_id_type=MESH
                )

    pairs = (
        (disp_h, first.at[:, 1 : X + 1]),
        (heat_h, heat),
        (diag_h, stiff.at[0:3]),
        (off_h, stiff.at[3:6]),
        (load_h, load),
        (clear_h, clear),
        (touch_h, touch),
        (clip_h, clip),
    )
    arriving = [pltpu.make_async_copy(s, d, in_sem.at[i]) for i, (s, d) in enumerate(pairs)]
    for copy in arriving:
        copy.start()

    row = lax.broadcasted_iota(jnp.int32, (Y, Z), 0)
    lane = lax.broadcasted_iota(jnp.int32, (Y, Z), 1)
    crow = lax.broadcasted_iota(jnp.int32, (h, w), 0)
    clane = lax.broadcasted_iota(jnp.int32, (h, w), 1)
    slane = lax.broadcasted_iota(jnp.int32, (Y, w), 1)
    own, mid = pl.ds(RING * X2, X2), pl.ds(h, h)

    def fine_ref(k):
        return first if k == 0 else fine.at[FINE.index(k) - 1]

    for way, (axis, there, has) in enumerate(ways):

        @pl.when(jnp.logical_not(has))
        def _():
            for k in SENT:
                if way >= 2:
                    yr[FINE.index(k), way - 2] = jnp.zeros(yr.shape[2:], jnp.float32)
                else:
                    fhalo[way] = jnp.zeros((Y, Z), jnp.float32)
                    for c in range(3):
                        fine_ref(k)[c, 0 if way == 0 else X + 1] = jnp.zeros((Y, Z), jnp.float32)

    for n, (di, dj) in enumerate(AROUND):

        @pl.when(jnp.logical_not(around[n]))
        def _():
            for ref, fill in ((kring, (1.0,) * 3 + (0.0,) * 3), (gring, (0.0,) * 3 + (FREE,))):
                for c, x in enumerate(fill):
                    if n in DIAGONAL:
                        spot = kfrom if ref is kring else gfrom
                        spot[DIAGONAL.index(n), c] = jnp.full((h, w), x, jnp.float32)
                    else:
                        for j in range(X2):
                            ref[c, (di + RING) * X2 + j, pl.ds((dj + 1) * h, h)] = jnp.full((h, w), x, jnp.float32)
            if n in NEXT:
                for c in range(3):
                    low[c, di + RING, pl.ds((dj + 1) * h, h)] = jnp.zeros((h, w), jnp.float32)

    def transfer(k, way, p=0):
        m = FINE.index(k)
        if way >= 2:
            src, dst = ys.at[m, way - 2], yr.at[m, 3 - way]
        else:
            part = pl.ds(p * H, H)
            src = edge.at[m, way, :, part]
            dst = fine_ref(k).at[:, 0 if way else X + 1, part]
        axis, there, _ = ways[way]
        return pltpu.make_async_remote_copy(
            src_ref=src,
            dst_ref=dst,
            send_sem=send_sem.at[m, way, p],
            recv_sem=recv_sem.at[m, way ^ 1, p],
            device_id={axis: there},
            device_id_type=MESH,
        )

    def begin(k, sides=(0, 1, 2, 3), p=0):
        for way in sides:

            @pl.when(ways[way][2])
            def _():
                transfer(k, way, p).start()

    def arrive(k, sides, p=0):
        for side in sides:

            @pl.when(ways[side][2])
            def _():
                transfer(k, side ^ 1, p).wait_recv()

    def leave(k):
        for way in range(4):

            @pl.when(ways[way][2])
            def _():
                for p in range(PIECES if way < 2 else 1):
                    transfer(k, way, p).wait_send()

    def ring_copy(kind, n):
        di, dj = AROUND[n]
        m = OPPOSITE[n]
        if n in DIAGONAL:
            src = (ksend, gsend)[kind].at[0 if dj < 0 else 1]
            dst = (kfrom, gfrom)[kind].at[DIAGONAL.index(m)]
        else:
            ref = (kring, gring, kring)[kind]
            part = pl.ds(0, ref.shape[0])
            if ref is kring and n in SIDES:
                part = pl.ds(3 if kind == CROSS else 0, 3)
            src = ref.at[part, own, mid]
            dst = ref.at[part, pl.ds((RING - di) * X2, X2), pl.ds((1 - dj) * h, h)]
        return pltpu.make_async_remote_copy(
            src_ref=src,
            dst_ref=dst,
            send_sem=ring_send.at[kind, n],
            recv_sem=ring_recv.at[kind, m],
            device_id={"grp": g + di, "brick": b + dj},
            device_id_type=MESH,
        )

    def low_copy(n):
        di, dj = AROUND[n]
        return pltpu.make_async_remote_copy(
            src_ref=low.at[:, RING, mid],
            dst_ref=low.at[:, RING - di, pl.ds((1 - dj) * h, h)],
            send_sem=low_send.at[n],
            recv_sem=low_recv.at[OPPOSITE[n]],
            device_id={"grp": g + di, "brick": b + dj},
            device_id_type=MESH,
        )

    def free_copy(way):
        axis, there, _ = ways[way]
        return pltpu.make_async_remote_copy(
            src_ref=fedge.at[way],
            dst_ref=fhalo.at[1 - way],
            send_sem=free_send.at[way],
            recv_sem=free_recv.at[1 - way],
            device_id={axis: there},
            device_id_type=MESH,
        )

    def ring_begin(copy, which):
        for n in which:

            @pl.when(around[n])
            def _():
                copy(n).start()

    def ring_arrive(copy, which):
        for n in which:

            @pl.when(around[n])
            def _():
                copy(OPPOSITE[n]).wait_recv()

    def ring_leave(copy, which):
        for n in which:

            @pl.when(around[n])
            def _():
                copy(n).wait_send()

    def corners_pack(ref, out, count):
        for c in range(count):
            near, far = ref[c, RING * X2, mid], ref[c, RING * X2 + X2 - 1, mid]
            out[0, c] = jnp.where(crow < h // 2, near, pltpu.roll(far, h // 2, 0))
            out[1, c] = jnp.where(crow < h // 2, pltpu.roll(near, h // 2, 0), far)

    def corners_unpack(out, ref, count):
        for d, n in enumerate(DIAGONAL):
            di, dj = AROUND[n]
            rows = pl.ds((dj + 1) * h, h)
            for c in range(count):
                x = out[d, c]
                y = pltpu.roll(x, h // 2, 0)
                ref[c, (di + RING) * X2, rows] = y if dj < 0 else x
                ref[c, (di + RING) * X2 + X2 - 1, rows] = x if dj < 0 else y

    def edge_rows(k, layers, c, i, v):
        n = c * layers + i
        m = FINE.index(k)
        ys[m, 0, n : n + 1, :] = v[0:1, :]
        ys[m, 1, n : n + 1, :] = v[Y - 1 : Y, :]

    def before(v, s):
        at = lane if v.shape[1] == Z else clane
        return jnp.where(at < s, 0.0, pltpu.roll(v, s, 1))

    def after(v, s):
        at = lane if v.shape[1] == Z else clane
        size = v.shape[1]
        return jnp.where(at >= size - s, 0.0, pltpu.roll(v, size - s, 1))

    def above(k, layers, c, i, v, s):
        n = c * layers + i
        return jnp.where(row < s, yr[FINE.index(k), 0, n : n + 1, :], pltpu.roll(v, s, 0))

    def below(k, layers, c, i, v, s):
        n = c * layers + i
        return jnp.where(row >= Y - s, yr[FINE.index(k), 1, n : n + 1, :], pltpu.roll(v, Y - s, 0))

    def shrink(slot, v, how):
        v = how(v, pltpu.roll(v, Z - 1, 1))
        spots = (2 * slane) & (w - 1)
        lo = jnp.take_along_axis(v[:, 0:w], spots, axis=1)
        hi = jnp.take_along_axis(v[:, w:Z], spots, axis=1)
        squeezed[slot] = jnp.where(slane < w // 2, lo, hi)
        return how(squeezed[slot, pl.ds(0, h, stride=2), :], squeezed[slot, pl.ds(1, h, stride=2), :])

    def grow(slot, x):
        squeezed[slot, pl.ds(0, h, stride=2), :] = x
        squeezed[slot, pl.ds(1, h, stride=2), :] = x
        return widen(squeezed[slot])

    def widen(v):
        spots = slane >> 1
        parts = [jnp.take_along_axis(v, spots + n * (w // 2), axis=1) for n in (0, 1)]
        return jnp.concatenate(parts, 1)

    def pair(v, axis, how):
        size = v.shape[axis]
        at = (crow, clane)[axis]
        return how(v, jnp.where((at & 1) == 0, pltpu.roll(v, size - 1, axis), pltpu.roll(v, 1, axis)))

    def group(v, w, how):
        return pair(pair(how(v, w), 1, how), 0, how)

    def plus(v, w):
        return v + w

    def layer(ref, i, count=3):
        return [ref[c, i] for c in range(count)]

    def put(ref, i, values):
        for c, v in enumerate(values):
            ref[c, i] = v

    def relaxed(v, inv, rest, obstacle):
        step = symmetric_times(inv, rest)
        w = [v[c] + OMEGA * step[c] for c in range(3)]
        return [jnp.minimum(w[0], obstacle), w[1], w[2]]

    def opened(inv, right, obstacle):
        w = [OMEGA * x for x in symmetric_times(inv, right)]
        return [jnp.minimum(w[0], obstacle), w[1], w[2]]

    def fine_stage(k, finish):
        ref, m = fine_ref(k), FINE.index(k)
        for i in range(X):
            v = layer(ref, i + 1)
            kv = symmetric_times(layer(stiff, i, 6), v)
            for c in range(3):
                near = jnp.where(row < 1, 0.0, pltpu.roll(v[c], 1, 0))
                near = near + jnp.where(row >= Y - 1, 0.0, pltpu.roll(v[c], Y - 1, 0))
                near = near + (before(v[c], 1) + after(v[c], 1))
                r = (force[c, i] - kv[c]) + near
                for n in (i - 1, i + 1):
                    if 0 <= n < X:
                        r = r + ref[c, n + 1]
                rests[c, i] = r
        if k in SENT[1:]:
            arrive(k, (2, 3))
        for i in range(X):
            for c in range(3):
                n = c * X + i
                rests[c, i, 0:1, :] = rests[c, i, 0:1, :] + yr[m, 0, n : n + 1, :]
                rests[c, i, Y - 1 : Y, :] = rests[c, i, Y - 1 : Y, :] + yr[m, 1, n : n + 1, :]
        for i in range(1, X - 1):
            for p in range(PIECES):
                finish(i, p, [rests[c, i, pl.ds(p * H, H)] for c in range(3)])
        for p in range(PIECES):
            part = pl.ds(p * H, H)
            for side, i in ((0, 0), (1, X - 1)):
                if k in SENT:
                    arrive(k, (side,), p)
                rest = [rests[c, i, part] + ref[c, (X + 1) * side, part] for c in range(3)]
                if X == 1 and side == 0:
                    for c in range(3):
                        rests[c, i, part] = rest[c]
                else:
                    finish(i, p, rest)

    def leave_edge(k, side, p, w):
        part = pl.ds(p * H, H)
        h = heat[(X - 1) * side, part]
        edge[FINE.index(k), side, 0, part] = w[0] + h if side else w[0] - h
        for c in (1, 2):
            edge[FINE.index(k), side, c, part] = w[c]
        begin(k, (side,), p)

    def fine_store(to, i, p, w):
        for c in range(3):
            fine_ref(to)[c, i + 1, pl.ds(p * H, H)] = w[c]
        for side, end in ((0, 0), (1, X - 1)):
            if i == end:
                leave_edge(to, side, p, w)
        for c in range(3):
            n = c * X + i
            if p == 0:
                ys[FINE.index(to), 0, n : n + 1, :] = w[c][0:1, :]
            if p == PIECES - 1:
                ys[FINE.index(to), 1, n : n + 1, :] = w[c][H - 1 : H, :]

    def fine_sweep(k, to):
        def finish(i, p, rest):
            part = pl.ds(p * H, H)
            v = [fine_ref(k)[c, i + 1, part] for c in range(3)]
            w = relaxed(v, [inv1[c, i, part] for c in range(6)], rest, obst1[i, part])
            fine_store(to, i, p, w)
            if to == 10:
                for c in range(3):
                    moved[c, i, part] = w[c]

        fine_stage(k, finish)
        begin(to, (2, 3))

    arriving[0].wait()
    arriving[1].wait()
    pl.semaphore_wait(barrier, sum(jnp.where(has, 1, 0) for has in around))
    for p in range(PIECES):
        for side in (0, 1):
            leave_edge(0, side, p, [first[c, 1 + (X - 1) * side, pl.ds(p * H, H)] for c in range(3)])
    for i in range(X):
        for c in range(3):
            edge_rows(0, X, c, i, first[c, i + 1])
        edge_rows(0, X, 3, i, heat[i])
    begin(0, (2, 3))
    for copy in arriving[2:]:
        copy.wait()
    for i in range(X):
        put(inv1, i, inverse(layer(stiff, i, 6)))
        obst1[i] = jnp.where(touch[i] == 1, clear[i], FREE)
    arrive(0, (2, 3))
    for i in range(X):
        warm = heat[i]
        along = load[0, i]
        if i > 0:
            along = along + heat[i - 1]
        if i < X - 1:
            along = along - heat[i + 1]
        force[0, i] = along
        force[1, i] = load[1, i] - (below(0, X, 3, i, warm, 1) - above(0, X, 3, i, warm, 1))
        force[2, i] = load[2, i] - (after(warm, 1) - before(warm, 1))

    for j in range(X2):
        for c in range(6):
            both = stiff[c, 2 * j] + stiff[c, 2 * j + 1]
            kring[c, RING * X2 + j, mid] = 0.125 * shrink(6 * j + c, both, plus)
    blocks_copy, rights_copy, cross_copy = (
        lambda n: ring_copy(BLOCKS, n),
        lambda n: ring_copy(RIGHTS, n),
        lambda n: ring_copy(CROSS, n),
    )
    corners_pack(kring, ksend, 6)
    ring_begin(blocks_copy, SIDES + REST)
    for i in range(X):
        free[i] = jnp.where(clip[i] == 1, 0.0, 1.0)
        ys[FINE.index(1), 0, 3 * X + i : 3 * X + i + 1, :] = free[i, 0:1, :]
        ys[FINE.index(1), 1, 3 * X + i : 3 * X + i + 1, :] = free[i, Y - 1 : Y, :]
    for side in (0, 1):
        fedge[side] = free[(X - 1) * side]
    fine_sweep(0, 1)
    ring_begin(cross_copy, SIDES)
    fine_sweep(1, 2)
    ring_begin(blocks_copy, CLOSE)

    def block(ref, i, t, count=3):
        return [ref[c, i, t * h : t * h + h, :] for c in range(count)]

    def block_put(ref, i, t, values):
        for c, x in enumerate(values):
            ref[c, i, t * h : t * h + h, :] = x

    first_own = RING * X2
    last_own = first_own + X2 - 1

    def region(straight, sideways):
        spots = [(i, 1) for i in range(first_own - straight, last_own + straight + 1)]
        for t in (0, 2):
            spots += [(i, t) for i in range(first_own - sideways, last_own + sideways + 1)]
        return spots

    def keep(di, dj):
        if (di, dj) == (0, 0):
            return None
        return jnp.where(around[AROUND.index((di, dj))], 1.0, 0.0)

    for j in range(X2):
        gaps = []
        for i in (2 * j, 2 * j + 1):
            allowed = (touch[i] == 1) & (clip[i] == 0)
            gaps.append(jnp.where(allowed, clear[i] - fine_ref(2)[0, i + 1], FREE))
        gring[3, first_own + j, mid] = shrink(j, jnp.minimum(gaps[0], gaps[1]), jnp.minimum)
    fine_rests = {}

    def restrict(i, p, rest):
        fine_rests[i, p] = [jnp.where(clip[i, pl.ds(p * H, H)] == 1, 0.0, rest[0]), rest[1], rest[2]]
        j = i // 2
        if all((n, q) in fine_rests for n in (2 * j, 2 * j + 1) for q in range(PIECES)):
            for c in range(3):
                both = [fine_rests[2 * j, q][c] + fine_rests[2 * j + 1, q][c] for q in range(PIECES)]
                right = 0.25 * shrink(X2 + 3 * j + c, jnp.concatenate(both, 0), plus)
                gring[c, first_own + j, mid] = right

    fine_stage(2, restrict)
    ring_begin(rights_copy, [n for n in STRAIGHT if abs(AROUND[n][0]) == 1])
    corners_pack(gring, gsend, 4)
    ring_begin(rights_copy, DIAGONAL)
    ring_begin(rights_copy, [n for n in STRAIGHT if abs(AROUND[n][0]) != 1])
    for way in (0, 1):

        @pl.when(ways[way][2])
        def _():
            free_copy(way).start()

    ring_arrive(blocks_copy, range(len(AROUND)))
    ring_arrive(cross_copy, SIDES)
    corners_unpack(kfrom, kring, 6)
    for i, t in region(4, 3):
        block_put(iring, i, t, inverse(block(kring, i, t, 6), keep(i // X2 - RING, t - 1)))
    thirds = [(0, 1), (1, 1), (2, 1), (1, 0), (1, 2)]
    base = first_own - 2
    k3 = None
    for n, (q, t) in enumerate(thirds):
        pairs = [block(kring, base + 2 * q + e, t, 6) for e in (0, 1)]
        k = [0.125 * group(pairs[0][c], pairs[1][c], plus) for c in range(6)]
        if (q, t) == (1, 1):
            k3 = k
        for c, x in enumerate(inverse(k, keep(q - 1, t - 1))):
            inv3[n, c] = x
    for c in range(6):
        inv3[len(thirds), c] = k3[c]

    ring_arrive(rights_copy, range(len(AROUND)))
    corners_unpack(gfrom, gring, 4)

    def ring_rest(m, i, t):
        v = block(m, i, t)
        kv = symmetric_times(block(kring, i, t, 6), v)
        right = block(gring, i, t)
        rest = []
        for c in range(3):
            up = m[c, i, t * h - 1 : t * h + h - 1, :] if t > 0 else pltpu.roll(v[c], 1, 0)
            down = m[c, i, t * h + 1 : t * h + h + 1, :] if t < 2 else pltpu.roll(v[c], h - 1, 0)
            near = (up + down) + (before(v[c], 1) + after(v[c], 1))
            near = near + (m[c, i - 1, t * h : t * h + h, :] + m[c, i + 1, t * h : t * h + h, :])
            rest.append((right[c] - kv[c]) + near)
        return rest

    def ring_sweep(m, i, t):
        obstacle = gring[3, i, t * h : t * h + h, :]
        return relaxed(block(m, i, t), block(iring, i, t, 6), ring_rest(m, i, t), obstacle)

    for i, t in region(4, 3):
        obstacle = gring[3, i, t * h : t * h + h, :]
        block_put(m0, i, t, opened(block(iring, i, t, 6), block(gring, i, t), obstacle))
    for i, t in region(3, 2):
        block_put(m1, i, t, ring_sweep(m0, i, t))
    g3 = obst3 = None
    for n, (q, t) in enumerate(thirds):
        spots = (base + 2 * q, base + 2 * q + 1)
        rest = [ring_rest(m1, i, t) for i in spots]
        right = [0.25 * group(rest[0][c], rest[1][c], plus) for c in range(3)]
        gaps = [gring[3, i, t * h : t * h + h, :] - m1[0, i, t * h : t * h + h, :] for i in spots]
        obstacle = group(gaps[0], gaps[1], jnp.minimum)
        if (q, t) == (1, 1):
            g3, obst3 = right, obstacle
        block_put(m4, q, t, opened([inv3[n, c] for c in range(6)], right, obstacle))
    v = block(m4, 1, 1)
    kv = symmetric_times([inv3[len(thirds), c] for c in range(6)], v)
    rest = []
    for c in range(3):
        near = m4[c, 1, h - 2 : 2 * h - 2, :] + m4[c, 1, h + 2 : 2 * h + 2, :]
        near = near + (before(v[c], 2) + after(v[c], 2)) + (m4[c, 0, h : 2 * h, :] + m4[c, 2, h : 2 * h, :])
        rest.append((g3[c] - kv[c]) + near)
    block_put(low, RING, 1, relaxed(v, [inv3[1, c] for c in range(6)], rest, obst3))
    ring_begin(low_copy, NEXT)
    ring_arrive(low_copy, NEXT)
    for i, t in region(3, 2):
        lows = block(low, i // X2, t)
        block_put(m2, i, t, [x + y for x, y in zip(block(m1, i, t), lows)])
    for i, t in region(2, 1):
        block_put(m3, i, t, ring_sweep(m2, i, t))
    for i, t in region(1, 0):
        block_put(m0, i, t, ring_sweep(m3, i, t))
    for j in range(X2):
        lift = [grow(3 * j + c, x) for c, x in enumerate(block(m0, first_own + j, 1))]
        for i in (2 * j, 2 * j + 1):
            old = layer(fine_ref(2), i + 1)
            put(fine_ref(8), i + 1, [old[0] + free[i] * lift[0], old[1] + lift[1], old[2] + lift[2]])
    for way in (0, 1):

        @pl.when(ways[way][2])
        def _():
            free_copy(way ^ 1).wait_recv()

    for side, i in ((0, first_own - 1), (1, last_own + 1)):
        lift = [grow(3 * (X2 + side) + c, x) for c, x in enumerate(block(m0, i, 1))]
        old = layer(fine_ref(2), (X + 1) * side)
        put(fine_ref(8), (X + 1) * side, [old[0] + fhalo[side] * lift[0], old[1] + lift[1], old[2] + lift[2]])
    spots = [(side, c, j) for side in (0, 1) for c in range(3) for j in range(X2)]
    top = 3 * (X2 + 2)
    for n, (side, c, j) in enumerate(spots):
        at = 2 * h if side else h - 1
        squeezed[top + n // Y, n % Y : n % Y + 1, :] = m0[c, first_own + j, at : at + 1, :]
    last = FINE.index(2)
    for n, (side, c, j) in enumerate(spots):
        if n % Y == 0:
            lift = widen(squeezed[top + n // Y])
        line = lift[n % Y : n % Y + 1, :]
        for i in (2 * j, 2 * j + 1):
            x = line
            if c == 0:
                x = line * yr[FINE.index(1), side, 3 * X + i : 3 * X + i + 1, :]
            yr[FINE.index(8), side, c * X + i : c * X + i + 1, :] = (
                yr[last, side, c * X + i : c * X + i + 1, :] + x
            )
    fine_sweep(8, 9)
    fine_sweep(9, 10)

    def remain(i, p, rest):
        for c in range(3):
            resid[c, i, pl.ds(p * H, H)] = rest[c]

    fine_stage(10, remain)
    for k in SENT:
        leave(k)
    for way in (0, 1):

        @pl.when(ways[way][2])
        def _():
            free_copy(way).wait_send()

    ring_leave(cross_copy, SIDES)
    ring_leave(blocks_copy, range(len(AROUND)))
    ring_leave(rights_copy, range(len(AROUND)))
    ring_leave(low_copy, NEXT)


def local(*args):
    disp, _, heat = args[:3]
    X, Y, Z = heat.shape
    X2 = X // 2
    h, w = Y // 2, Z // 2
    f32 = jnp.float32

    def buffer(*shape, dtype=f32):
        return pltpu.VMEM(shape + (Y, Z), dtype)

    def small(*shape):
        return pltpu.VMEM(shape + (w,), f32)

    rows = -(-4 * X // 8) * 8
    layers, tall, corners = (2 * RING + 1) * X2, 3 * h, len(DIAGONAL)
    scratch = [
        buffer(3, X + 2),
        buffer(X),
        buffer(5, 3, X + 2),
        buffer(len(FINE), 2, 3),
        pltpu.VMEM((len(FINE), 2, rows, Z), f32),
        pltpu.VMEM((len(FINE), 2, rows, Z), f32),
        buffer(3, X),
        buffer(6, X),
        buffer(X),
        buffer(X, dtype=jnp.int32),
        buffer(X, dtype=jnp.int32),
        buffer(3, X),
        buffer(3, X),
        buffer(6, X),
        buffer(X),
        small(3 * (X2 + 2) - (-6 * X2 // Y), Y),
        small(6, layers, tall),
        small(4, layers, tall),
        small(6, layers, tall),
        small(2, 6, h),
        small(corners, 6, h),
        small(2, 4, h),
        small(corners, 4, h),
        small(3, layers, tall),
        small(3, layers, tall),
        small(3, layers, tall),
        small(3, layers, tall),
        small(6, 6, h),
        small(3, 3, tall),
        small(3, 2 * RING + 1, tall),
        buffer(X),
        buffer(2),
        buffer(2),
        pltpu.SemaphoreType.DMA((8,)),
        pltpu.SemaphoreType.DMA((len(FINE), 4, PIECES)),
        pltpu.SemaphoreType.DMA((len(FINE), 4, PIECES)),
        pltpu.SemaphoreType.DMA((3, len(AROUND))),
        pltpu.SemaphoreType.DMA((3, len(AROUND))),
        pltpu.SemaphoreType.DMA((len(AROUND),)),
        pltpu.SemaphoreType.DMA((len(AROUND),)),
        pltpu.SemaphoreType.DMA((2,)),
        pltpu.SemaphoreType.DMA((2,)),
    ]
    anywhere = pl.BlockSpec(memory_space=pl.ANY)
    return pl.pallas_call(
        kernel,
        out_shape=[pltpu.VMEM(disp.shape, f32)] * 2,
        in_specs=[anywhere] * 8,
        out_specs=[pl.BlockSpec(memory_space=pltpu.VMEM)] * 2,
        scratch_shapes=scratch,
        compiler_params=pltpu.CompilerParams(collective_id=0, has_side_effects=True),
        name="vcycle",
    )(*args)


def solution(mesh):
    whole = P(None, "grp", "brick", None)
    flat = P("grp", "brick", None)
    return jax.shard_map(
        local,
        mesh=mesh,
        in_specs=(whole, whole, flat, whole, whole, flat, flat, flat),
        out_specs=(whole, whole),
        check_vma=False,
    )
```

```python
import jax
import jax.numpy as jnp
from jax import lax
from jax.experimental import pallas as pl
from jax.experimental.pallas import tpu as pltpu
from jax.sharding import PartitionSpec as P

OMEGA = 0.6
FREE = 1000.0
FINE = (0, 1, 2, 8, 9, 10)
PIECES = 2
RING = 2
AROUND = [(1, 0), (-1, 0), (1, 1), (1, -1), (-1, 1), (-1, -1), (2, 0), (-2, 0)]
AROUND += [(0, 1), (0, -1), (2, 1), (2, -1), (-2, 1), (-2, -1)]
STRAIGHT = [n for n, (di, dj) in enumerate(AROUND) if not (di and dj)]
DIAGONAL = [n for n, (di, dj) in enumerate(AROUND) if di and dj]
NEXT = [n for n, (di, dj) in enumerate(AROUND) if abs(di) < 2 or dj == 0]
SIDES = [AROUND.index((1, 0)), AROUND.index((-1, 0))]
CLOSE = [n for n in DIAGONAL if abs(AROUND[n][0]) == 1]
REST = [n for n in range(len(AROUND)) if n not in SIDES + CLOSE]
SENT = (0, 1, 2, 9, 10)
OPPOSITE = [AROUND.index((-di, -dj)) for di, dj in AROUND]
BLOCKS, RIGHTS, CROSS = 0, 1, 2
MESH = pl.DeviceIdType.MESH


def inverse(k, keep=None):
    a, b, c, d, e, f = k
    i00 = b * c - e * e
    i11 = a * c - f * f
    i22 = a * b - d * d
    i01 = f * e - d * c
    i12 = d * f - a * e
    i02 = d * e - b * f
    scale = 1.0 / (a * i00 + d * i01 + f * i02)
    if keep is not None:
        scale = scale * keep
    return [i00 * scale, i11 * scale, i22 * scale, i01 * scale, i12 * scale, i02 * scale]


def symmetric_times(m, v):
    return [
        m[0] * v[0] + m[3] * v[1] + m[5] * v[2],
        m[3] * v[0] + m[1] * v[1] + m[4] * v[2],
        m[5] * v[0] + m[4] * v[1] + m[2] * v[2],
    ]


def kernel(
    disp_h, load_h, heat_h, diag_h, off_h, clear_h, touch_h, clip_h,
    moved, resid,
    first, heat, fine, edge, ys, yr, load, stiff, clear, touch, clip,
    force, rests, inv1, obst1,
    squeezed, kring, gring, iring, ksend, kfrom, gsend, gfrom, m0, m1, m2, m3, inv3, m4, low,
    free, fedge, fhalo,
    in_sem, send_sem, recv_sem, ring_send, ring_recv, low_send, low_recv, free_send, free_recv,
):
    X, Y, Z = heat_h.shape
    X2, X3 = X // 2, X // 4
    H = Y // PIECES
    h, w = Y // 2, Z // 2
    g, b = lax.axis_index("grp"), lax.axis_index("brick")
    ng, nb = lax.axis_size("grp"), lax.axis_size("brick")
    ways = (
        ("grp", g - 1, g > 0),
        ("grp", g + 1, g < ng - 1),
        ("brick", b - 1, b > 0),
        ("brick", b + 1, b < nb - 1),
    )
    barrier = pltpu.get_barrier_semaphore()
    for axis, there, has in ways:

        @pl.when(has)
        def _():
            pl.semaphore_signal(barrier, inc=1, device_id={axis: there}, device_id_type=MESH)

    def reaches(di, dj):
        has = None
        for d, at, count in ((di, g, ng), (dj, b, nb)):
            if d:
                inside = at + d >= 0 if d < 0 else at + d < count
                has = inside if has is None else has & inside
        return has

    around = [reaches(di, dj) for di, dj in AROUND]
    for (di, dj), has in zip(AROUND, around):
        if abs(di) + abs(dj) > 1:

            @pl.when(has)
            def _():
                pl.semaphore_signal(
                    barrier, inc=1, device_id={"grp": g + di, "brick": b + dj}, device_id_type=MESH
                )

    pairs = (
        (disp_h, first.at[:, 1 : X + 1]),
        (heat_h, heat),
        (diag_h, stiff.at[0:3]),
        (off_h, stiff.at[3:6]),
        (load_h, load),
        (clear_h, clear),
        (touch_h, touch),
        (clip_h, clip),
    )
    arriving = [pltpu.make_async_copy(s, d, in_sem.at[i]) for i, (s, d) in enumerate(pairs)]
    for copy in arriving:
        copy.start()

    row = lax.broadcasted_iota(jnp.int32, (Y, Z), 0)
    lane = lax.broadcasted_iota(jnp.int32, (Y, Z), 1)
    crow = lax.broadcasted_iota(jnp.int32, (h, w), 0)
    clane = lax.broadcasted_iota(jnp.int32, (h, w), 1)
    slane = lax.broadcasted_iota(jnp.int32, (Y, w), 1)
    own, mid = pl.ds(RING * X2, X2), pl.ds(h, h)

    def fine_ref(k):
        return first if k == 0 else fine.at[FINE.index(k) - 1]

    for way, (axis, there, has) in enumerate(ways):

        @pl.when(jnp.logical_not(has))
        def _():
            for k in SENT:
                if way >= 2:
                    yr[FINE.index(k), way - 2] = jnp.zeros(yr.shape[2:], jnp.float32)
                else:
                    fhalo[way] = jnp.zeros((Y, Z), jnp.float32)
                    for c in range(3):
                        fine_ref(k)[c, 0 if way == 0 else X + 1] = jnp.zeros((Y, Z), jnp.float32)

    for n, (di, dj) in enumerate(AROUND):

        @pl.when(jnp.logical_not(around[n]))
        def _():
            for ref, fill in ((kring, (1.0,) * 3 + (0.0,) * 3), (gring, (0.0,) * 3 + (FREE,))):
                for c, x in enumerate(fill):
                    if n in DIAGONAL:
                        spot = kfrom if ref is kring else gfrom
                        spot[DIAGONAL.index(n), c] = jnp.full((h, w), x, jnp.float32)
                    else:
                        for j in range(X2):
                            ref[c, (di + RING) * X2 + j, pl.ds((dj + 1) * h, h)] = jnp.full((h, w), x, jnp.float32)
            if n in NEXT:
                for c in range(3):
                    low[c, di + RING, pl.ds((dj + 1) * h, h)] = jnp.zeros((h, w), jnp.float32)

    def transfer(k, way, p=0):
        m = FINE.index(k)
        if way >= 2:
            src, dst = ys.at[m, way - 2], yr.at[m, 3 - way]
        else:
            part = pl.ds(p * H, H)
            src = edge.at[m, way, :, part]
            dst = fine_ref(k).at[:, 0 if way else X + 1, part]
        axis, there, _ = ways[way]
        return pltpu.make_async_remote_copy(
            src_ref=src,
            dst_ref=dst,
            send_sem=send_sem.at[m, way, p],
            recv_sem=recv_sem.at[m, way ^ 1, p],
            device_id={axis: there},
            device_id_type=MESH,
        )

    def begin(k, sides=(0, 1, 2, 3), p=0):
        for way in sides:

            @pl.when(ways[way][2])
            def _():
                transfer(k, way, p).start()

    def arrive(k, sides, p=0):
        for side in sides:

            @pl.when(ways[side][2])
            def _():
                transfer(k, side ^ 1, p).wait_recv()

    def leave(k):
        for way in range(4):

            @pl.when(ways[way][2])
            def _():
                for p in range(PIECES if way < 2 else 1):
                    transfer(k, way, p).wait_send()

    def ring_copy(kind, n):
        di, dj = AROUND[n]
        m = OPPOSITE[n]
        if n in DIAGONAL:
            src = (ksend, gsend)[kind].at[0 if dj < 0 else 1]
            dst = (kfrom, gfrom)[kind].at[DIAGONAL.index(m)]
        else:
            ref = (kring, gring, kring)[kind]
            part = pl.ds(0, ref.shape[0])
            if ref is kring and n in SIDES:
                part = pl.ds(3 if kind == CROSS else 0, 3)
            src = ref.at[part, own, mid]
            dst = ref.at[part, pl.ds((RING - di) * X2, X2), pl.ds((1 - dj) * h, h)]
        return pltpu.make_async_remote_copy(
            src_ref=src,
            dst_ref=dst,
            send_sem=ring_send.at[kind, n],
            recv_sem=ring_recv.at[kind, m],
            device_id={"grp": g + di, "brick": b + dj},
            device_id_type=MESH,
        )

    def low_copy(n):
        di, dj = AROUND[n]
        return pltpu.make_async_remote_copy(
            src_ref=low.at[:, RING, mid],
            dst_ref=low.at[:, RING - di, pl.ds((1 - dj) * h, h)],
            send_sem=low_send.at[n],
            recv_sem=low_recv.at[OPPOSITE[n]],
            device_id={"grp": g + di, "brick": b + dj},
            device_id_type=MESH,
        )

    def free_copy(way):
        axis, there, _ = ways[way]
        return pltpu.make_async_remote_copy(
            src_ref=fedge.at[way],
            dst_ref=fhalo.at[1 - way],
            send_sem=free_send.at[way],
            recv_sem=free_recv.at[1 - way],
            device_id={axis: there},
            device_id_type=MESH,
        )

    def ring_begin(copy, which):
        for n in which:

            @pl.when(around[n])
            def _():
                copy(n).start()

    def ring_arrive(copy, which):
        for n in which:

            @pl.when(around[n])
            def _():
                copy(OPPOSITE[n]).wait_recv()

    def ring_leave(copy, which):
        for n in which:

            @pl.when(around[n])
            def _():
                copy(n).wait_send()

    def corners_pack(ref, out, count):
        for c in range(count):
            near, far = ref[c, RING * X2, mid], ref[c, RING * X2 + X2 - 1, mid]
            out[0, c] = jnp.where(crow < h // 2, near, pltpu.roll(far, h // 2, 0))
            out[1, c] = jnp.where(crow < h // 2, pltpu.roll(near, h // 2, 0), far)

    def corners_unpack(out, ref, count):
        for d, n in enumerate(DIAGONAL):
            di, dj = AROUND[n]
            rows = pl.ds((dj + 1) * h, h)
            for c in range(count):
                x = out[d, c]
                y = pltpu.roll(x, h // 2, 0)
                ref[c, (di + RING) * X2, rows] = y if dj < 0 else x
                ref[c, (di + RING) * X2 + X2 - 1, rows] = x if dj < 0 else y

    def edge_rows(k, layers, c, i, v):
        n = c * layers + i
        m = FINE.index(k)
        ys[m, 0, n : n + 1, :] = v[0:1, :]
        ys[m, 1, n : n + 1, :] = v[Y - 1 : Y, :]

    def before(v, s):
        at = lane if v.shape[1] == Z else clane
        return jnp.where(at < s, 0.0, pltpu.roll(v, s, 1))

    def after(v, s):
        at = lane if v.shape[1] == Z else clane
        size = v.shape[1]
        return jnp.where(at >= size - s, 0.0, pltpu.roll(v, size - s, 1))

    def above(k, layers, c, i, v, s):
        n = c * layers + i
        return jnp.where(row < s, yr[FINE.index(k), 0, n : n + 1, :], pltpu.roll(v, s, 0))

    def below(k, layers, c, i, v, s):
        n = c * layers + i
        return jnp.where(row >= Y - s, yr[FINE.index(k), 1, n : n + 1, :], pltpu.roll(v, Y - s, 0))

    def shrink(slot, v, how):
        v = how(v, pltpu.roll(v, Z - 1, 1))
        spots = (2 * slane) & (w - 1)
        lo = jnp.take_along_axis(v[:, 0:w], spots, axis=1)
        hi = jnp.take_along_axis(v[:, w:Z], spots, axis=1)
        squeezed[slot] = jnp.where(slane < w // 2, lo, hi)
        return how(squeezed[slot, pl.ds(0, h, stride=2), :], squeezed[slot, pl.ds(1, h, stride=2), :])

    def grow(slot, x):
        squeezed[slot, pl.ds(0, h, stride=2), :] = x
        squeezed[slot, pl.ds(1, h, stride=2), :] = x
        return widen(squeezed[slot])

    def widen(v):
        spots = slane >> 1
        parts = [jnp.take_along_axis(v, spots + n * (w // 2), axis=1) for n in (0, 1)]
        return jnp.concatenate(parts, 1)

    def pair(v, axis, how):
        size = v.shape[axis]
        at = (crow, clane)[axis]
        return how(v, jnp.where((at & 1) == 0, pltpu.roll(v, size - 1, axis), pltpu.roll(v, 1, axis)))

    def group(v, w, how):
        return pair(pair(how(v, w), 1, how), 0, how)

    def plus(v, w):
        return v + w

    def layer(ref, i, count=3):
        return [ref[c, i] for c in range(count)]

    def put(ref, i, values):
        for c, v in enumerate(values):
            ref[c, i] = v

    def relaxed(v, inv, rest, obstacle):
        step = symmetric_times(inv, rest)
        w = [v[c] + OMEGA * step[c] for c in range(3)]
        return [jnp.minimum(w[0], obstacle), w[1], w[2]]

    def opened(inv, right, obstacle):
        w = [OMEGA * x for x in symmetric_times(inv, right)]
        return [jnp.minimum(w[0], obstacle), w[1], w[2]]

    def fine_stage(k, finish):
        ref, m = fine_ref(k), FINE.index(k)
        for i in sorted(range(X), key=lambda i: i not in (0, X - 1)):
            v = layer(ref, i + 1)
            kv = symmetric_times(layer(stiff, i, 6), v)
            for c in range(3):
                near = jnp.where(row < 1, 0.0, pltpu.roll(v[c], 1, 0))
                near = near + jnp.where(row >= Y - 1, 0.0, pltpu.roll(v[c], Y - 1, 0))
                near = near + (before(v[c], 1) + after(v[c], 1))
                r = (force[c, i] - kv[c]) + near
                for n in (i - 1, i + 1):
                    if 0 <= n < X:
                        r = r + ref[c, n + 1]
                rests[c, i] = r
        if k in SENT[1:]:
            arrive(k, (2, 3))
        for i in range(X):
            for c in range(3):
                n = c * X + i
                rests[c, i, 0:1, :] = rests[c, i, 0:1, :] + yr[m, 0, n : n + 1, :]
                rests[c, i, Y - 1 : Y, :] = rests[c, i, Y - 1 : Y, :] + yr[m, 1, n : n + 1, :]

        def inside():
            for i in range(1, X - 1):
                for p in range(PIECES):
                    finish(i, p, [rests[c, i, pl.ds(p * H, H)] for c in range(3)])

        if k in SENT:
            inside()
        if k == SENT[-1]:
            leave_all()
        for p in range(PIECES):
            part = pl.ds(p * H, H)
            for side, i in ((0, 0), (1, X - 1)):
                if k in SENT:
                    arrive(k, (side,), p)
                rest = [rests[c, i, part] + ref[c, (X + 1) * side, part] for c in range(3)]
                if X == 1 and side == 0:
                    for c in range(3):
                        rests[c, i, part] = rest[c]
                else:
                    finish(i, p, rest)
        if k not in SENT:
            inside()

    def leave_edge(k, side, p, w):
        part = pl.ds(p * H, H)
        h = heat[(X - 1) * side, part]
        edge[FINE.index(k), side, 0, part] = w[0] + h if side else w[0] - h
        for c in (1, 2):
            edge[FINE.index(k), side, c, part] = w[c]
        begin(k, (side,), p)

    def fine_store(to, i, p, w):
        for c in range(3):
            fine_ref(to)[c, i + 1, pl.ds(p * H, H)] = w[c]
        for side, end in ((0, 0), (1, X - 1)):
            if i == end:
                leave_edge(to, side, p, w)
        for c in range(3):
            n = c * X + i
            if p == 0:
                ys[FINE.index(to), 0, n : n + 1, :] = w[c][0:1, :]
            if p == PIECES - 1:
                ys[FINE.index(to), 1, n : n + 1, :] = w[c][H - 1 : H, :]

    def fine_sweep(k, to):
        def finish(i, p, rest):
            part = pl.ds(p * H, H)
            v = [fine_ref(k)[c, i + 1, part] for c in range(3)]
            w = relaxed(v, [inv1[c, i, part] for c in range(6)], rest, obst1[i, part])
            fine_store(to, i, p, w)
            if to == 10:
                for c in range(3):
                    moved[c, i, part] = w[c]

        fine_stage(k, finish)
        begin(to, (2, 3))

    arriving[0].wait()
    arriving[1].wait()
    pl.semaphore_wait(barrier, sum(jnp.where(has, 1, 0) for has in around))
    for p in range(PIECES):
        for side in (0, 1):
            leave_edge(0, side, p, [first[c, 1 + (X - 1) * side, pl.ds(p * H, H)] for c in range(3)])
    for i in range(X):
        for c in range(3):
            edge_rows(0, X, c, i, first[c, i + 1])
        edge_rows(0, X, 3, i, heat[i])
    begin(0, (2, 3))
    for copy in arriving[2:]:
        copy.wait()
    for i in range(X):
        put(inv1, i, inverse(layer(stiff, i, 6)))
        obst1[i] = jnp.where(touch[i] == 1, clear[i], FREE)
    arrive(0, (2, 3))
    for i in range(X):
        warm = heat[i]
        along = load[0, i]
        if i > 0:
            along = along + heat[i - 1]
        if i < X - 1:
            along = along - heat[i + 1]
        force[0, i] = along
        force[1, i] = load[1, i] - (below(0, X, 3, i, warm, 1) - above(0, X, 3, i, warm, 1))
        force[2, i] = load[2, i] - (after(warm, 1) - before(warm, 1))

    for j in range(X2):
        for c in range(6):
            both = stiff[c, 2 * j] + stiff[c, 2 * j + 1]
            kring[c, RING * X2 + j, mid] = 0.125 * shrink(6 * j + c, both, plus)
    blocks_copy, rights_copy, cross_copy = (
        lambda n: ring_copy(BLOCKS, n),
        lambda n: ring_copy(RIGHTS, n),
        lambda n: ring_copy(CROSS, n),
    )
    corners_pack(kring, ksend, 6)
    ring_begin(blocks_copy, SIDES + REST)
    for i in range(X):
        free[i] = jnp.where(clip[i] == 1, 0.0, 1.0)
        ys[FINE.index(1), 0, 3 * X + i : 3 * X + i + 1, :] = free[i, 0:1, :]
        ys[FINE.index(1), 1, 3 * X + i : 3 * X + i + 1, :] = free[i, Y - 1 : Y, :]
    for side in (0, 1):
        fedge[side] = free[(X - 1) * side]
    fine_sweep(0, 1)
    ring_begin(cross_copy, SIDES)
    fine_sweep(1, 2)
    ring_begin(blocks_copy, CLOSE)

    def block(ref, i, t, count=3):
        return [ref[c, i, t * h : t * h + h, :] for c in range(count)]

    def block_put(ref, i, t, values):
        for c, x in enumerate(values):
            ref[c, i, t * h : t * h + h, :] = x

    first_own = RING * X2
    last_own = first_own + X2 - 1

    def region(straight, sideways):
        spots = [(i, 1) for i in range(first_own - straight, last_own + straight + 1)]
        for t in (0, 2):
            spots += [(i, t) for i in range(first_own - sideways, last_own + sideways + 1)]
        return spots

    def keep(di, dj):
        if (di, dj) == (0, 0):
            return None
        return jnp.where(around[AROUND.index((di, dj))], 1.0, 0.0)

    for j in range(X2):
        gaps = []
        for i in (2 * j, 2 * j + 1):
            allowed = (touch[i] == 1) & (clip[i] == 0)
            gaps.append(jnp.where(allowed, clear[i] - fine_ref(2)[0, i + 1], FREE))
        gring[3, first_own + j, mid] = shrink(j, jnp.minimum(gaps[0], gaps[1]), jnp.minimum)
    fine_rests = {}

    def restrict(i, p, rest):
        fine_rests[i, p] = [jnp.where(clip[i, pl.ds(p * H, H)] == 1, 0.0, rest[0]), rest[1], rest[2]]
        j = i // 2
        if all((n, q) in fine_rests for n in (2 * j, 2 * j + 1) for q in range(PIECES)):
            for c in range(3):
                both = [fine_rests[2 * j, q][c] + fine_rests[2 * j + 1, q][c] for q in range(PIECES)]
                right = 0.25 * shrink(X2 + 3 * j + c, jnp.concatenate(both, 0), plus)
                gring[c, first_own + j, mid] = right

    fine_stage(2, restrict)
    ring_begin(rights_copy, [n for n in STRAIGHT if abs(AROUND[n][0]) == 1])
    corners_pack(gring, gsend, 4)
    ring_begin(rights_copy, DIAGONAL)
    ring_begin(rights_copy, [n for n in STRAIGHT if abs(AROUND[n][0]) != 1])
    for way in (0, 1):

        @pl.when(ways[way][2])
        def _():
            free_copy(way).start()

    ring_arrive(blocks_copy, range(len(AROUND)))
    ring_arrive(cross_copy, SIDES)
    corners_unpack(kfrom, kring, 6)
    for i, t in region(4, 3):
        block_put(iring, i, t, inverse(block(kring, i, t, 6), keep(i // X2 - RING, t - 1)))
    thirds = [(0, 1), (1, 1), (2, 1), (1, 0), (1, 2)]
    base = first_own - 2
    k3 = None
    for n, (q, t) in enumerate(thirds):
        pairs = [block(kring, base + 2 * q + e, t, 6) for e in (0, 1)]
        k = [0.125 * group(pairs[0][c], pairs[1][c], plus) for c in range(6)]
        if (q, t) == (1, 1):
            k3 = k
        for c, x in enumerate(inverse(k, keep(q - 1, t - 1))):
            inv3[n, c] = x
    for c in range(6):
        inv3[len(thirds), c] = k3[c]

    ring_arrive(rights_copy, range(len(AROUND)))
    corners_unpack(gfrom, gring, 4)

    def ring_rest(m, i, t):
        v = block(m, i, t)
        kv = symmetric_times(block(kring, i, t, 6), v)
        right = block(gring, i, t)
        rest = []
        for c in range(3):
            up = m[c, i, t * h - 1 : t * h + h - 1, :] if t > 0 else pltpu.roll(v[c], 1, 0)
            down = m[c, i, t * h + 1 : t * h + h + 1, :] if t < 2 else pltpu.roll(v[c], h - 1, 0)
            near = (up + down) + (before(v[c], 1) + after(v[c], 1))
            near = near + (m[c, i - 1, t * h : t * h + h, :] + m[c, i + 1, t * h : t * h + h, :])
            rest.append((right[c] - kv[c]) + near)
        return rest

    def ring_sweep(m, i, t):
        obstacle = gring[3, i, t * h : t * h + h, :]
        return relaxed(block(m, i, t), block(iring, i, t, 6), ring_rest(m, i, t), obstacle)

    for i, t in region(4, 3):
        obstacle = gring[3, i, t * h : t * h + h, :]
        block_put(m0, i, t, opened(block(iring, i, t, 6), block(gring, i, t), obstacle))
    for i, t in region(3, 2):
        block_put(m1, i, t, ring_sweep(m0, i, t))
    g3 = obst3 = None
    for n, (q, t) in enumerate(thirds):
        spots = (base + 2 * q, base + 2 * q + 1)
        rest = [ring_rest(m1, i, t) for i in spots]
        right = [0.25 * group(rest[0][c], rest[1][c], plus) for c in range(3)]
        gaps = [gring[3, i, t * h : t * h + h, :] - m1[0, i, t * h : t * h + h, :] for i in spots]
        obstacle = group(gaps[0], gaps[1], jnp.minimum)
        if (q, t) == (1, 1):
            g3, obst3 = right, obstacle
        block_put(m4, q, t, opened([inv3[n, c] for c in range(6)], right, obstacle))
    v = block(m4, 1, 1)
    kv = symmetric_times([inv3[len(thirds), c] for c in range(6)], v)
    rest = []
    for c in range(3):
        near = m4[c, 1, h - 2 : 2 * h - 2, :] + m4[c, 1, h + 2 : 2 * h + 2, :]
        near = near + (before(v[c], 2) + after(v[c], 2)) + (m4[c, 0, h : 2 * h, :] + m4[c, 2, h : 2 * h, :])
        rest.append((g3[c] - kv[c]) + near)
    block_put(low, RING, 1, relaxed(v, [inv3[1, c] for c in range(6)], rest, obst3))
    ring_begin(low_copy, NEXT)
    ring_arrive(low_copy, NEXT)
    for i, t in region(3, 2):
        lows = block(low, i // X2, t)
        block_put(m2, i, t, [x + y for x, y in zip(block(m1, i, t), lows)])
    for i, t in region(2, 1):
        block_put(m3, i, t, ring_sweep(m2, i, t))
    for i, t in region(1, 0):
        block_put(m0, i, t, ring_sweep(m3, i, t))
    for j in range(X2):
        lift = [grow(3 * j + c, x) for c, x in enumerate(block(m0, first_own + j, 1))]
        for i in (2 * j, 2 * j + 1):
            old = layer(fine_ref(2), i + 1)
            put(fine_ref(8), i + 1, [old[0] + free[i] * lift[0], old[1] + lift[1], old[2] + lift[2]])
    for way in (0, 1):

        @pl.when(ways[way][2])
        def _():
            free_copy(way ^ 1).wait_recv()

    for side, i in ((0, first_own - 1), (1, last_own + 1)):
        lift = [grow(3 * (X2 + side) + c, x) for c, x in enumerate(block(m0, i, 1))]
        old = layer(fine_ref(2), (X + 1) * side)
        put(fine_ref(8), (X + 1) * side, [old[0] + fhalo[side] * lift[0], old[1] + lift[1], old[2] + lift[2]])
    spots = [(side, c, j) for side in (0, 1) for c in range(3) for j in range(X2)]
    top = 3 * (X2 + 2)
    for n, (side, c, j) in enumerate(spots):
        at = 2 * h if side else h - 1
        squeezed[top + n // Y, n % Y : n % Y + 1, :] = m0[c, first_own + j, at : at + 1, :]
    last = FINE.index(2)
    for n, (side, c, j) in enumerate(spots):
        if n % Y == 0:
            lift = widen(squeezed[top + n // Y])
        line = lift[n % Y : n % Y + 1, :]
        for i in (2 * j, 2 * j + 1):
            x = line
            if c == 0:
                x = line * yr[FINE.index(1), side, 3 * X + i : 3 * X + i + 1, :]
            yr[FINE.index(8), side, c * X + i : c * X + i + 1, :] = (
                yr[last, side, c * X + i : c * X + i + 1, :] + x
            )
    fine_sweep(8, 9)
    fine_sweep(9, 10)

    def remain(i, p, rest):
        for c in range(3):
            resid[c, i, pl.ds(p * H, H)] = rest[c]

    def leave_all():
        for k in SENT[:-1]:
            leave(k)
        for way in (0, 1):

            @pl.when(ways[way][2])
            def _():
                free_copy(way).wait_send()

        ring_leave(cross_copy, SIDES)
        ring_leave(blocks_copy, range(len(AROUND)))
        ring_leave(rights_copy, range(len(AROUND)))
        ring_leave(low_copy, NEXT)

    fine_stage(10, remain)
    leave(SENT[-1])


def local(*args):
    disp, _, heat = args[:3]
    X, Y, Z = heat.shape
    X2 = X // 2
    h, w = Y // 2, Z // 2
    f32 = jnp.float32

    def buffer(*shape, dtype=f32):
        return pltpu.VMEM(shape + (Y, Z), dtype)

    def small(*shape):
        return pltpu.VMEM(shape + (w,), f32)

    rows = -(-4 * X // 8) * 8
    layers, tall, corners = (2 * RING + 1) * X2, 3 * h, len(DIAGONAL)
    scratch = [
        buffer(3, X + 2),
        buffer(X),
        buffer(5, 3, X + 2),
        buffer(len(FINE), 2, 3),
        pltpu.VMEM((len(FINE), 2, rows, Z), f32),
        pltpu.VMEM((len(FINE), 2, rows, Z), f32),
        buffer(3, X),
        buffer(6, X),
        buffer(X),
        buffer(X, dtype=jnp.int32),
        buffer(X, dtype=jnp.int32),
        buffer(3, X),
        buffer(3, X),
        buffer(6, X),
        buffer(X),
        small(3 * (X2 + 2) - (-6 * X2 // Y), Y),
        small(6, layers, tall),
        small(4, layers, tall),
        small(6, layers, tall),
        small(2, 6, h),
        small(corners, 6, h),
        small(2, 4, h),
        small(corners, 4, h),
        small(3, layers, tall),
        small(3, layers, tall),
        small(3, layers, tall),
        small(3, layers, tall),
        small(6, 6, h),
        small(3, 3, tall),
        small(3, 2 * RING + 1, tall),
        buffer(X),
        buffer(2),
        buffer(2),
        pltpu.SemaphoreType.DMA((8,)),
        pltpu.SemaphoreType.DMA((len(FINE), 4, PIECES)),
        pltpu.SemaphoreType.DMA((len(FINE), 4, PIECES)),
        pltpu.SemaphoreType.DMA((3, len(AROUND))),
        pltpu.SemaphoreType.DMA((3, len(AROUND))),
        pltpu.SemaphoreType.DMA((len(AROUND),)),
        pltpu.SemaphoreType.DMA((len(AROUND),)),
        pltpu.SemaphoreType.DMA((2,)),
        pltpu.SemaphoreType.DMA((2,)),
    ]
    anywhere = pl.BlockSpec(memory_space=pl.ANY)
    return pl.pallas_call(
        kernel,
        out_shape=[pltpu.VMEM(disp.shape, f32)] * 2,
        in_specs=[anywhere] * 8,
        out_specs=[pl.BlockSpec(memory_space=pltpu.VMEM)] * 2,
        scratch_shapes=scratch,
        compiler_params=pltpu.CompilerParams(collective_id=0, has_side_effects=True),
        name="vcycle",
    )(*args)


def solution(mesh):
    whole = P(None, "grp", "brick", None)
    flat = P("grp", "brick", None)
    return jax.shard_map(
        local,
        mesh=mesh,
        in_specs=(whole, whole, flat, whole, whole, flat, flat, flat),
        out_specs=(whole, whole),
        check_vma=False,
    )
```

```python
import jax
import jax.numpy as jnp
from jax import lax
from jax.experimental import pallas as pl
from jax.experimental.pallas import tpu as pltpu
from jax.sharding import PartitionSpec as P

OMEGA = 0.6
FREE = 1000.0
FINE = (0, 1, 2, 8, 9, 10)
PIECES = 2
RING = 2
AROUND = [(1, 0), (-1, 0), (1, 1), (1, -1), (-1, 1), (-1, -1), (2, 0), (-2, 0)]
AROUND += [(0, 1), (0, -1), (2, 1), (2, -1), (-2, 1), (-2, -1)]
STRAIGHT = [n for n, (di, dj) in enumerate(AROUND) if not (di and dj)]
DIAGONAL = [n for n, (di, dj) in enumerate(AROUND) if di and dj]
NEXT = [n for n, (di, dj) in enumerate(AROUND) if abs(di) < 2 or dj == 0]
SIDES = [AROUND.index((1, 0)), AROUND.index((-1, 0))]
CLOSE = [n for n in DIAGONAL if abs(AROUND[n][0]) == 1]
REST = [n for n in range(len(AROUND)) if n not in SIDES + CLOSE]
SENT = (0, 1, 2, 9, 10)
OPPOSITE = [AROUND.index((-di, -dj)) for di, dj in AROUND]
BLOCKS, RIGHTS, CROSS = 0, 1, 2
MESH = pl.DeviceIdType.MESH


def inverse(k, keep=None):
    a, b, c, d, e, f = k
    i00 = b * c - e * e
    i11 = a * c - f * f
    i22 = a * b - d * d
    i01 = f * e - d * c
    i12 = d * f - a * e
    i02 = d * e - b * f
    scale = 1.0 / (a * i00 + d * i01 + f * i02)
    if keep is not None:
        scale = scale * keep
    return [i00 * scale, i11 * scale, i22 * scale, i01 * scale, i12 * scale, i02 * scale]


def symmetric_times(m, v):
    return [
        m[0] * v[0] + m[3] * v[1] + m[5] * v[2],
        m[3] * v[0] + m[1] * v[1] + m[4] * v[2],
        m[5] * v[0] + m[4] * v[1] + m[2] * v[2],
    ]


def kernel(
    disp_h, load_h, heat_h, diag_h, off_h, clear_h, touch_h, clip_h,
    moved, resid,
    first, heat, fine, edge, ys, yr, load, stiff, clear, touch, clip,
    force, rests, inv1, obst1,
    squeezed, kring, gring, iring, ksend, kfrom, gsend, gfrom, m0, m1, m2, m3, inv3, m4, low,
    free, fedge, fhalo,
    in_sem, send_sem, recv_sem, ring_send, ring_recv, low_send, low_recv, free_send, free_recv,
):
    X, Y, Z = heat_h.shape
    X2, X3 = X // 2, X // 4
    H = Y // PIECES
    h, w = Y // 2, Z // 2
    g, b = lax.axis_index("grp"), lax.axis_index("brick")
    ng, nb = lax.axis_size("grp"), lax.axis_size("brick")
    ways = (
        ("grp", g - 1, g > 0),
        ("grp", g + 1, g < ng - 1),
        ("brick", b - 1, b > 0),
        ("brick", b + 1, b < nb - 1),
    )
    barrier = pltpu.get_barrier_semaphore()
    for axis, there, has in ways:

        @pl.when(has)
        def _():
            pl.semaphore_signal(barrier, inc=1, device_id={axis: there}, device_id_type=MESH)

    def reaches(di, dj):
        has = None
        for d, at, count in ((di, g, ng), (dj, b, nb)):
            if d:
                inside = at + d >= 0 if d < 0 else at + d < count
                has = inside if has is None else has & inside
        return has

    around = [reaches(di, dj) for di, dj in AROUND]
    for (di, dj), has in zip(AROUND, around):
        if abs(di) + abs(dj) > 1:

            @pl.when(has)
            def _():
                pl.semaphore_signal(
                    barrier, inc=1, device_id={"grp": g + di, "brick": b + dj}, device_id_type=MESH
                )

    pairs = (
        (disp_h, first.at[:, 1 : X + 1]),
        (heat_h, heat),
        (diag_h, stiff.at[0:3]),
        (off_h, stiff.at[3:6]),
        (load_h, load),
        (clear_h, clear),
        (touch_h, touch),
        (clip_h, clip),
    )
    arriving = [pltpu.make_async_copy(s, d, in_sem.at[i]) for i, (s, d) in enumerate(pairs)]
    for copy in arriving:
        copy.start()

    row = lax.broadcasted_iota(jnp.int32, (Y, Z), 0)
    lane = lax.broadcasted_iota(jnp.int32, (Y, Z), 1)
    crow = lax.broadcasted_iota(jnp.int32, (h, w), 0)
    clane = lax.broadcasted_iota(jnp.int32, (h, w), 1)
    slane = lax.broadcasted_iota(jnp.int32, (Y, w), 1)
    own, mid = pl.ds(RING * X2, X2), pl.ds(h, h)

    def fine_ref(k):
        return first if k == 0 else fine.at[FINE.index(k) - 1]

    for way, (axis, there, has) in enumerate(ways):

        @pl.when(jnp.logical_not(has))
        def _():
            for k in SENT:
                if way >= 2:
                    yr[FINE.index(k), way - 2] = jnp.zeros(yr.shape[2:], jnp.float32)
                else:
                    fhalo[way] = jnp.zeros((Y, Z), jnp.float32)
                    for c in range(3):
                        fine_ref(k)[c, 0 if way == 0 else X + 1] = jnp.zeros((Y, Z), jnp.float32)

    for n, (di, dj) in enumerate(AROUND):

        @pl.when(jnp.logical_not(around[n]))
        def _():
            for ref, fill in ((kring, (1.0,) * 3 + (0.0,) * 3), (gring, (0.0,) * 3 + (FREE,))):
                for c, x in enumerate(fill):
                    if n in DIAGONAL:
                        spot = kfrom if ref is kring else gfrom
                        spot[DIAGONAL.index(n), c] = jnp.full((h, w), x, jnp.float32)
                    else:
                        for j in range(X2):
                            ref[c, (di + RING) * X2 + j, pl.ds((dj + 1) * h, h)] = jnp.full((h, w), x, jnp.float32)
            if n in NEXT:
                for c in range(3):
                    low[c, di + RING, pl.ds((dj + 1) * h, h)] = jnp.zeros((h, w), jnp.float32)

    def transfer(k, way, p=0):
        m = FINE.index(k)
        if way >= 2:
            src, dst = ys.at[m, way - 2], yr.at[m, 3 - way]
        else:
            part = pl.ds(p * H, H)
            src = edge.at[m, way, :, part]
            dst = fine_ref(k).at[:, 0 if way else X + 1, part]
        axis, there, _ = ways[way]
        return pltpu.make_async_remote_copy(
            src_ref=src,
            dst_ref=dst,
            send_sem=send_sem.at[m, way, p],
            recv_sem=recv_sem.at[m, way ^ 1, p],
            device_id={axis: there},
            device_id_type=MESH,
        )

    def begin(k, sides=(0, 1, 2, 3), p=0):
        for way in sides:

            @pl.when(ways[way][2])
            def _():
                transfer(k, way, p).start()

    def arrive(k, sides, p=0):
        for side in sides:

            @pl.when(ways[side][2])
            def _():
                transfer(k, side ^ 1, p).wait_recv()

    def leave(k):
        for way in range(4):

            @pl.when(ways[way][2])
            def _():
                for p in range(PIECES if way < 2 else 1):
                    transfer(k, way, p).wait_send()

    def ring_copy(kind, n):
        di, dj = AROUND[n]
        m = OPPOSITE[n]
        if n in DIAGONAL:
            src = (ksend, gsend)[kind].at[0 if dj < 0 else 1]
            dst = (kfrom, gfrom)[kind].at[DIAGONAL.index(m)]
        else:
            ref = (kring, gring, kring)[kind]
            part = pl.ds(0, ref.shape[0])
            if ref is kring and n in SIDES:
                part = pl.ds(3 if kind == CROSS else 0, 3)
            src = ref.at[part, own, mid]
            dst = ref.at[part, pl.ds((RING - di) * X2, X2), pl.ds((1 - dj) * h, h)]
        return pltpu.make_async_remote_copy(
            src_ref=src,
            dst_ref=dst,
            send_sem=ring_send.at[kind, n],
            recv_sem=ring_recv.at[kind, m],
            device_id={"grp": g + di, "brick": b + dj},
            device_id_type=MESH,
        )

    def low_copy(n):
        di, dj = AROUND[n]
        return pltpu.make_async_remote_copy(
            src_ref=low.at[:, RING, mid],
            dst_ref=low.at[:, RING - di, pl.ds((1 - dj) * h, h)],
            send_sem=low_send.at[n],
            recv_sem=low_recv.at[OPPOSITE[n]],
            device_id={"grp": g + di, "brick": b + dj},
            device_id_type=MESH,
        )

    def free_copy(way):
        axis, there, _ = ways[way]
        return pltpu.make_async_remote_copy(
            src_ref=fedge.at[way],
            dst_ref=fhalo.at[1 - way],
            send_sem=free_send.at[way],
            recv_sem=free_recv.at[1 - way],
            device_id={axis: there},
            device_id_type=MESH,
        )

    def ring_begin(copy, which):
        for n in which:

            @pl.when(around[n])
            def _():
                copy(n).start()

    def ring_arrive(copy, which):
        for n in which:

            @pl.when(around[n])
            def _():
                copy(OPPOSITE[n]).wait_recv()

    def ring_leave(copy, which):
        for n in which:

            @pl.when(around[n])
            def _():
                copy(n).wait_send()

    def corners_pack(ref, out, count):
        for c in range(count):
            near, far = ref[c, RING * X2, mid], ref[c, RING * X2 + X2 - 1, mid]
            out[0, c] = jnp.where(crow < h // 2, near, pltpu.roll(far, h // 2, 0))
            out[1, c] = jnp.where(crow < h // 2, pltpu.roll(near, h // 2, 0), far)

    def corners_unpack(out, ref, count):
        for d, n in enumerate(DIAGONAL):
            di, dj = AROUND[n]
            rows = pl.ds((dj + 1) * h, h)
            for c in range(count):
                x = out[d, c]
                y = pltpu.roll(x, h // 2, 0)
                ref[c, (di + RING) * X2, rows] = y if dj < 0 else x
                ref[c, (di + RING) * X2 + X2 - 1, rows] = x if dj < 0 else y

    def edge_rows(k, layers, c, i, v):
        n = c * layers + i
        m = FINE.index(k)
        ys[m, 0, n : n + 1, :] = v[0:1, :]
        ys[m, 1, n : n + 1, :] = v[Y - 1 : Y, :]

    def before(v, s):
        at = lane if v.shape[1] == Z else clane
        return jnp.where(at < s, 0.0, pltpu.roll(v, s, 1))

    def after(v, s):
        at = lane if v.shape[1] == Z else clane
        size = v.shape[1]
        return jnp.where(at >= size - s, 0.0, pltpu.roll(v, size - s, 1))

    def above(k, layers, c, i, v, s):
        n = c * layers + i
        return jnp.where(row < s, yr[FINE.index(k), 0, n : n + 1, :], pltpu.roll(v, s, 0))

    def below(k, layers, c, i, v, s):
        n = c * layers + i
        return jnp.where(row >= Y - s, yr[FINE.index(k), 1, n : n + 1, :], pltpu.roll(v, Y - s, 0))

    def shrink(slot, v, how):
        v = how(v, pltpu.roll(v, Z - 1, 1))
        spots = (2 * slane) & (w - 1)
        lo = jnp.take_along_axis(v[:, 0:w], spots, axis=1)
        hi = jnp.take_along_axis(v[:, w:Z], spots, axis=1)
        squeezed[slot] = jnp.where(slane < w // 2, lo, hi)
        return how(squeezed[slot, pl.ds(0, h, stride=2), :], squeezed[slot, pl.ds(1, h, stride=2), :])

    def grow(slot, x):
        squeezed[slot, pl.ds(0, h, stride=2), :] = x
        squeezed[slot, pl.ds(1, h, stride=2), :] = x
        return widen(squeezed[slot])

    def widen(v):
        spots = slane >> 1
        parts = [jnp.take_along_axis(v, spots + n * (w // 2), axis=1) for n in (0, 1)]
        return jnp.concatenate(parts, 1)

    def pair(v, axis, how):
        size = v.shape[axis]
        at = (crow, clane)[axis]
        return how(v, jnp.where((at & 1) == 0, pltpu.roll(v, size - 1, axis), pltpu.roll(v, 1, axis)))

    def group(v, w, how):
        return pair(pair(how(v, w), 1, how), 0, how)

    def plus(v, w):
        return v + w

    def layer(ref, i, count=3):
        return [ref[c, i] for c in range(count)]

    def put(ref, i, values):
        for c, v in enumerate(values):
            ref[c, i] = v

    def relaxed(v, inv, rest, obstacle):
        step = symmetric_times(inv, rest)
        w = [v[c] + OMEGA * step[c] for c in range(3)]
        return [jnp.minimum(w[0], obstacle), w[1], w[2]]

    def opened(inv, right, obstacle):
        w = [OMEGA * x for x in symmetric_times(inv, right)]
        return [jnp.minimum(w[0], obstacle), w[1], w[2]]

    def fine_stage(k, finish):
        ref, m = fine_ref(k), FINE.index(k)
        for i in sorted(range(X), key=lambda i: i not in (0, X - 1)):
            v = layer(ref, i + 1)
            kv = symmetric_times(layer(stiff, i, 6), v)
            for c in range(3):
                near = jnp.where(row < 1, 0.0, pltpu.roll(v[c], 1, 0))
                near = near + jnp.where(row >= Y - 1, 0.0, pltpu.roll(v[c], Y - 1, 0))
                near = near + (before(v[c], 1) + after(v[c], 1))
                r = (force[c, i] - kv[c]) + near
                for n in (i - 1, i + 1):
                    if 0 <= n < X:
                        r = r + ref[c, n + 1]
                rests[c, i] = r
        if k in SENT[1:]:
            arrive(k, (2, 3))
        for i in range(X):
            for c in range(3):
                n = c * X + i
                rests[c, i, 0:1, :] = rests[c, i, 0:1, :] + yr[m, 0, n : n + 1, :]
                rests[c, i, Y - 1 : Y, :] = rests[c, i, Y - 1 : Y, :] + yr[m, 1, n : n + 1, :]

        def inside():
            for i in range(1, X - 1):
                for p in range(PIECES):
                    finish(i, p, [rests[c, i, pl.ds(p * H, H)] for c in range(3)])

        if k in SENT:
            inside()
        if k == SENT[-1]:
            leave_all()
        for p in range(PIECES):
            part = pl.ds(p * H, H)
            for side, i in ((0, 0), (1, X - 1)):
                if k in SENT:
                    arrive(k, (side,), p)
                rest = [rests[c, i, part] + ref[c, (X + 1) * side, part] for c in range(3)]
                if X == 1 and side == 0:
                    for c in range(3):
                        rests[c, i, part] = rest[c]
                else:
                    finish(i, p, rest)
        if k not in SENT:
            inside()

    def leave_edge(k, side, p, w):
        part = pl.ds(p * H, H)
        h = heat[(X - 1) * side, part]
        edge[FINE.index(k), side, 0, part] = w[0] + h if side else w[0] - h
        for c in (1, 2):
            edge[FINE.index(k), side, c, part] = w[c]
        begin(k, (side,), p)

    def fine_store(to, i, p, w):
        for c in range(3):
            fine_ref(to)[c, i + 1, pl.ds(p * H, H)] = w[c]
        for side, end in ((0, 0), (1, X - 1)):
            if i == end:
                leave_edge(to, side, p, w)
        for c in range(3):
            n = c * X + i
            if p == 0:
                ys[FINE.index(to), 0, n : n + 1, :] = w[c][0:1, :]
            if p == PIECES - 1:
                ys[FINE.index(to), 1, n : n + 1, :] = w[c][H - 1 : H, :]

    def fine_sweep(k, to):
        def finish(i, p, rest):
            part = pl.ds(p * H, H)
            v = [fine_ref(k)[c, i + 1, part] for c in range(3)]
            w = relaxed(v, [inv1[c, i, part] for c in range(6)], rest, obst1[i, part])
            fine_store(to, i, p, w)
            if to == 10:
                for c in range(3):
                    moved[c, i, part] = w[c]

        fine_stage(k, finish)
        begin(to, (2, 3))

    arriving[0].wait()
    arriving[1].wait()
    pl.semaphore_wait(barrier, sum(jnp.where(has, 1, 0) for has in around))
    for p in range(PIECES):
        for side in (0, 1):
            leave_edge(0, side, p, [first[c, 1 + (X - 1) * side, pl.ds(p * H, H)] for c in range(3)])
    for i in range(X):
        for c in range(3):
            edge_rows(0, X, c, i, first[c, i + 1])
        edge_rows(0, X, 3, i, heat[i])
    begin(0, (2, 3))
    for copy in arriving[2:]:
        copy.wait()
    for i in range(X):
        put(inv1, i, inverse(layer(stiff, i, 6)))
        obst1[i] = jnp.where(touch[i] == 1, clear[i], FREE)
    arrive(0, (2, 3))
    for i in range(X):
        warm = heat[i]
        along = load[0, i]
        if i > 0:
            along = along + heat[i - 1]
        if i < X - 1:
            along = along - heat[i + 1]
        force[0, i] = along
        force[1, i] = load[1, i] - (below(0, X, 3, i, warm, 1) - above(0, X, 3, i, warm, 1))
        force[2, i] = load[2, i] - (after(warm, 1) - before(warm, 1))

    for j in range(X2):
        for c in range(6):
            both = stiff[c, 2 * j] + stiff[c, 2 * j + 1]
            kring[c, RING * X2 + j, mid] = 0.125 * shrink(6 * j + c, both, plus)
    blocks_copy, rights_copy, cross_copy = (
        lambda n: ring_copy(BLOCKS, n),
        lambda n: ring_copy(RIGHTS, n),
        lambda n: ring_copy(CROSS, n),
    )
    corners_pack(kring, ksend, 6)
    ring_begin(blocks_copy, SIDES + REST)
    for i in range(X):
        free[i] = jnp.where(clip[i] == 1, 0.0, 1.0)
        ys[FINE.index(1), 0, 3 * X + i : 3 * X + i + 1, :] = free[i, 0:1, :]
        ys[FINE.index(1), 1, 3 * X + i : 3 * X + i + 1, :] = free[i, Y - 1 : Y, :]
    for side in (0, 1):
        fedge[side] = free[(X - 1) * side]
    fine_sweep(0, 1)
    ring_begin(cross_copy, SIDES)
    fine_sweep(1, 2)
    ring_begin(blocks_copy, CLOSE)

    def block(ref, i, t, count=3):
        return [ref[c, i, t * h : t * h + h, :] for c in range(count)]

    def block_put(ref, i, t, values):
        for c, x in enumerate(values):
            ref[c, i, t * h : t * h + h, :] = x

    first_own = RING * X2
    last_own = first_own + X2 - 1

    def region(straight, sideways):
        spots = [(i, 1) for i in range(first_own - straight, last_own + straight + 1)]
        for t in (0, 2):
            spots += [(i, t) for i in range(first_own - sideways, last_own + sideways + 1)]
        return spots

    def keep(di, dj):
        if (di, dj) == (0, 0):
            return None
        return jnp.where(around[AROUND.index((di, dj))], 1.0, 0.0)

    for j in range(X2):
        gaps = []
        for i in (2 * j, 2 * j + 1):
            allowed = (touch[i] == 1) & (clip[i] == 0)
            gaps.append(jnp.where(allowed, clear[i] - fine_ref(2)[0, i + 1], FREE))
        gring[3, first_own + j, mid] = shrink(j, jnp.minimum(gaps[0], gaps[1]), jnp.minimum)
    fine_rests = {}

    def restrict(i, p, rest):
        fine_rests[i, p] = [jnp.where(clip[i, pl.ds(p * H, H)] == 1, 0.0, rest[0]), rest[1], rest[2]]
        j = i // 2
        if all((n, q) in fine_rests for n in (2 * j, 2 * j + 1) for q in range(PIECES)):
            for c in range(3):
                both = [fine_rests[2 * j, q][c] + fine_rests[2 * j + 1, q][c] for q in range(PIECES)]
                right = 0.25 * shrink(X2 + 3 * j + c, jnp.concatenate(both, 0), plus)
                gring[c, first_own + j, mid] = right

    fine_stage(2, restrict)
    ring_begin(rights_copy, [n for n in STRAIGHT if abs(AROUND[n][0]) == 1])
    corners_pack(gring, gsend, 4)
    ring_begin(rights_copy, DIAGONAL)
    ring_begin(rights_copy, [n for n in STRAIGHT if abs(AROUND[n][0]) != 1])
    for way in (0, 1):

        @pl.when(ways[way][2])
        def _():
            free_copy(way).start()

    ring_arrive(blocks_copy, range(len(AROUND)))
    ring_arrive(cross_copy, SIDES)
    corners_unpack(kfrom, kring, 6)
    for i, t in region(4, 3):
        block_put(iring, i, t, inverse(block(kring, i, t, 6), keep(i // X2 - RING, t - 1)))
    thirds = [(0, 1), (1, 1), (2, 1), (1, 0), (1, 2)]
    base = first_own - 2
    k3 = None
    for n, (q, t) in enumerate(thirds):
        pairs = [block(kring, base + 2 * q + e, t, 6) for e in (0, 1)]
        k = [0.125 * group(pairs[0][c], pairs[1][c], plus) for c in range(6)]
        if (q, t) == (1, 1):
            k3 = k
        for c, x in enumerate(inverse(k, keep(q - 1, t - 1))):
            inv3[n, c] = x
    for c in range(6):
        inv3[len(thirds), c] = k3[c]

    ring_arrive(rights_copy, range(len(AROUND)))
    corners_unpack(gfrom, gring, 4)

    def ring_rest(m, i, t):
        v = block(m, i, t)
        kv = symmetric_times(block(kring, i, t, 6), v)
        right = block(gring, i, t)
        rest = []
        for c in range(3):
            up = m[c, i, t * h - 1 : t * h + h - 1, :] if t > 0 else pltpu.roll(v[c], 1, 0)
            down = m[c, i, t * h + 1 : t * h + h + 1, :] if t < 2 else pltpu.roll(v[c], h - 1, 0)
            near = (up + down) + (before(v[c], 1) + after(v[c], 1))
            near = near + (m[c, i - 1, t * h : t * h + h, :] + m[c, i + 1, t * h : t * h + h, :])
            rest.append((right[c] - kv[c]) + near)
        return rest

    def ring_sweep(m, i, t):
        obstacle = gring[3, i, t * h : t * h + h, :]
        return relaxed(block(m, i, t), block(iring, i, t, 6), ring_rest(m, i, t), obstacle)

    for i, t in region(4, 3):
        obstacle = gring[3, i, t * h : t * h + h, :]
        block_put(m0, i, t, opened(block(iring, i, t, 6), block(gring, i, t), obstacle))
    for i, t in region(3, 2):
        block_put(m1, i, t, ring_sweep(m0, i, t))
    g3 = obst3 = None
    for n, (q, t) in enumerate(thirds):
        spots = (base + 2 * q, base + 2 * q + 1)
        rest = [ring_rest(m1, i, t) for i in spots]
        right = [0.25 * group(rest[0][c], rest[1][c], plus) for c in range(3)]
        gaps = [gring[3, i, t * h : t * h + h, :] - m1[0, i, t * h : t * h + h, :] for i in spots]
        obstacle = group(gaps[0], gaps[1], jnp.minimum)
        if (q, t) == (1, 1):
            g3, obst3 = right, obstacle
        block_put(m4, q, t, opened([inv3[n, c] for c in range(6)], right, obstacle))
    v = block(m4, 1, 1)
    kv = symmetric_times([inv3[len(thirds), c] for c in range(6)], v)
    rest = []
    for c in range(3):
        near = m4[c, 1, h - 2 : 2 * h - 2, :] + m4[c, 1, h + 2 : 2 * h + 2, :]
        near = near + (before(v[c], 2) + after(v[c], 2)) + (m4[c, 0, h : 2 * h, :] + m4[c, 2, h : 2 * h, :])
        rest.append((g3[c] - kv[c]) + near)
    block_put(low, RING, 1, relaxed(v, [inv3[1, c] for c in range(6)], rest, obst3))
    ring_begin(low_copy, NEXT)
    ring_arrive(low_copy, NEXT)
    for i, t in region(3, 2):
        lows = block(low, i // X2, t)
        block_put(m2, i, t, [x + y for x, y in zip(block(m1, i, t), lows)])
    for i, t in region(2, 1):
        block_put(m3, i, t, ring_sweep(m2, i, t))
    for i, t in region(1, 0):
        block_put(m0, i, t, ring_sweep(m3, i, t))
    for j in range(X2):
        lift = [grow(3 * j + c, x) for c, x in enumerate(block(m0, first_own + j, 1))]
        for i in (2 * j, 2 * j + 1):
            old = layer(fine_ref(2), i + 1)
            put(fine_ref(8), i + 1, [old[0] + free[i] * lift[0], old[1] + lift[1], old[2] + lift[2]])
    for way in (0, 1):

        @pl.when(ways[way][2])
        def _():
            free_copy(way ^ 1).wait_recv()

    for side, i in ((0, first_own - 1), (1, last_own + 1)):
        lift = [grow(3 * (X2 + side) + c, x) for c, x in enumerate(block(m0, i, 1))]
        old = layer(fine_ref(2), (X + 1) * side)
        put(fine_ref(8), (X + 1) * side, [old[0] + fhalo[side] * lift[0], old[1] + lift[1], old[2] + lift[2]])
    spots = [(side, c, j) for side in (0, 1) for c in range(3) for j in range(X2)]
    top = 3 * (X2 + 2)
    for n, (side, c, j) in enumerate(spots):
        at = 2 * h if side else h - 1
        squeezed[top + n // Y, n % Y : n % Y + 1, :] = m0[c, first_own + j, at : at + 1, :]
    last = FINE.index(2)
    for n, (side, c, j) in enumerate(spots):
        if n % Y == 0:
            lift = widen(squeezed[top + n // Y])
        line = lift[n % Y : n % Y + 1, :]
        for i in (2 * j, 2 * j + 1):
            x = line
            if c == 0:
                x = line * yr[FINE.index(1), side, 3 * X + i : 3 * X + i + 1, :]
            yr[FINE.index(8), side, c * X + i : c * X + i + 1, :] = (
                yr[last, side, c * X + i : c * X + i + 1, :] + x
            )
    fine_sweep(8, 9)
    fine_sweep(9, 10)

    def remain(i, p, rest):
        for c in range(3):
            resid[c, i, pl.ds(p * H, H)] = rest[c]

    def leave_all():
        for k in SENT[:-1]:
            leave(k)
        for way in (0, 1):

            @pl.when(ways[way][2])
            def _():
                free_copy(way).wait_send()

        ring_leave(cross_copy, SIDES)
        ring_leave(blocks_copy, range(len(AROUND)))
        ring_leave(rights_copy, range(len(AROUND)))
        ring_leave(low_copy, NEXT)

    fine_stage(10, remain)
    leave(SENT[-1])


def flush(moved, resid, moved_h, resid_h, sem):
    copies = [
        pltpu.make_async_copy(moved, moved_h, sem.at[0]),
        pltpu.make_async_copy(resid, resid_h, sem.at[1]),
    ]
    for copy in copies:
        copy.start()
    for copy in copies:
        copy.wait()


def local(*args):
    disp, _, heat = args[:3]
    X, Y, Z = heat.shape
    X2 = X // 2
    h, w = Y // 2, Z // 2
    f32 = jnp.float32

    def buffer(*shape, dtype=f32):
        return pltpu.VMEM(shape + (Y, Z), dtype)

    def small(*shape):
        return pltpu.VMEM(shape + (w,), f32)

    rows = -(-4 * X // 8) * 8
    layers, tall, corners = (2 * RING + 1) * X2, 3 * h, len(DIAGONAL)
    scratch = [
        buffer(3, X + 2),
        buffer(X),
        buffer(5, 3, X + 2),
        buffer(len(FINE), 2, 3),
        pltpu.VMEM((len(FINE), 2, rows, Z), f32),
        pltpu.VMEM((len(FINE), 2, rows, Z), f32),
        buffer(3, X),
        buffer(6, X),
        buffer(X),
        buffer(X, dtype=jnp.int32),
        buffer(X, dtype=jnp.int32),
        buffer(3, X),
        buffer(3, X),
        buffer(6, X),
        buffer(X),
        small(3 * (X2 + 2) - (-6 * X2 // Y), Y),
        small(6, layers, tall),
        small(4, layers, tall),
        small(6, layers, tall),
        small(2, 6, h),
        small(corners, 6, h),
        small(2, 4, h),
        small(corners, 4, h),
        small(3, layers, tall),
        small(3, layers, tall),
        small(3, layers, tall),
        small(3, layers, tall),
        small(6, 6, h),
        small(3, 3, tall),
        small(3, 2 * RING + 1, tall),
        buffer(X),
        buffer(2),
        buffer(2),
        pltpu.SemaphoreType.DMA((8,)),
        pltpu.SemaphoreType.DMA((len(FINE), 4, PIECES)),
        pltpu.SemaphoreType.DMA((len(FINE), 4, PIECES)),
        pltpu.SemaphoreType.DMA((3, len(AROUND))),
        pltpu.SemaphoreType.DMA((3, len(AROUND))),
        pltpu.SemaphoreType.DMA((len(AROUND),)),
        pltpu.SemaphoreType.DMA((len(AROUND),)),
        pltpu.SemaphoreType.DMA((2,)),
        pltpu.SemaphoreType.DMA((2,)),
    ]
    anywhere = pl.BlockSpec(memory_space=pl.ANY)
    outs = pl.pallas_call(
        kernel,
        out_shape=[pltpu.VMEM(disp.shape, f32)] * 2,
        in_specs=[anywhere] * 8,
        out_specs=[pl.BlockSpec(memory_space=pltpu.VMEM)] * 2,
        scratch_shapes=scratch,
        compiler_params=pltpu.CompilerParams(collective_id=0, has_side_effects=True),
        name="vcycle",
    )(*args)
    return pl.pallas_call(
        flush,
        out_shape=[jax.ShapeDtypeStruct(disp.shape, f32)] * 2,
        in_specs=[pl.BlockSpec(memory_space=pltpu.VMEM)] * 2,
        out_specs=[anywhere] * 2,
        scratch_shapes=[pltpu.SemaphoreType.DMA((2,))],
        name="flush",
    )(*[pltpu.with_memory_space_constraint(x, pltpu.VMEM) for x in outs])


def solution(mesh):
    whole = P(None, "grp", "brick", None)
    flat = P("grp", "brick", None)
    return jax.shard_map(
        local,
        mesh=mesh,
        in_specs=(whole, whole, flat, whole, whole, flat, flat, flat),
        out_specs=(whole, whole),
        check_vma=False,
    )
```
